128 devices in a mesh: gx: 32 (over y, z, core), gy: 4 (over x).
Axes of the slice: x: 4, y: 4, z: 4, core: 2. Of those that a mesh axis runs over, the one named last changes fastest.
Arguments:
- velocity: bfloat16 [3, 64, 16, 16, 512], P(None, 'gx', 'gy'), may hold values from -6 to 6
- part_pos: float32 [16384, 3, 128], P(('gx', 'gy')), may hold values from -1 to 1
- part_vel: float32 [16384, 3, 128], P(('gx', 'gy')), may hold values from -6 to 6
- part_coef: float32 [16384, 2, 128], P(('gx', 'gy')), may hold values from 0.3 to 3
- counts: int32 [16384], P(('gx', 'gy')), may hold values from 1 to 128
- dest: int32 [16384], P(('gx', 'gy')), may hold values from 0 to 3, as said below
- elem: int32 [16384], P(('gx', 'gy')), may hold values from 0 to 127, as said below
Outputs:
- drag: float32 [16384, 3, 128], P(('gx', 'gy'))
- source: float32 [3, 64, 16, 16, 512], P(None, 'gx', 'gy')
The draws below stay inside these ranges and needn't reach their ends.
Inputs may be any that keep to these rules, and one draw needn't show every extreme that they name: `dest`: every device sends exactly 32 blocks to each gy index. `elem`: on every owning device, each of its 128 elements receives exactly one block.
All inputs are finite; a program needn't handle non-finite values.
Results may differ from the reference program's by a relative error of at most 0.0003.
Values sent between devices are 32-bit elements; how exact they have to be, the bound alone decides.
No kernel may reach another device: no remote copies, remote signals or barrier semaphores. Data moves between devices by JAX's collectives and lax.ppermute only.
A program may use at most 128 MiB of HBM per device.

```python
import math
import jax
import jax.numpy as jnp
from jax import lax

EXD = 2
EYD = 4
EZ = 16
NODES = 512
SLOTS = 128
E_DEV = 128
NEX = 64
NEY = 16
NB = 16384
N_GX = 32
N_GY = 4


def joint_routes(key):
    share_size = E_DEV // N_GY

    def one_row(row_key):
        elem_keys = jax.random.split(jax.random.fold_in(row_key, 1), N_GY)
        mix_keys = jax.random.split(jax.random.fold_in(row_key, 2), N_GY)
        ladder = jnp.arange(E_DEV, dtype=jnp.int32)
        incoming = jax.vmap(lambda k: jax.random.permutation(k, ladder))(elem_keys)
        elements = incoming.reshape(N_GY, N_GY, share_size).transpose(1, 0, 2).reshape(N_GY, E_DEV)
        targets = jnp.broadcast_to(jnp.arange(N_GY, dtype=jnp.int32)[None, :, None], (N_GY, N_GY, share_size)).reshape(N_GY, E_DEV)
        shuffle = jax.vmap(lambda k: jax.random.permutation(k, ladder))(mix_keys)
        return (jnp.take_along_axis(targets, shuffle, axis=1), jnp.take_along_axis(elements, shuffle, axis=1))
    targets, elements = jax.vmap(one_row)(jax.random.split(key, N_GX))
    return (targets.reshape(-1), elements.reshape(-1))


def draw_dest(key, part):
    return joint_routes(jax.random.fold_in(key, 7))[0]


def draw_elem(key, part):
    return joint_routes(jax.random.fold_in(key, 7))[1]


def set_ends(result, stream_key, low, high):
    extent = result.shape
    spot = [jax.random.randint(jax.random.fold_in(stream_key, axis), (), 0, extent[axis]) for axis in range(len(extent))]
    result = result.at[tuple(spot)].set(low)
    longest = extent.index(max(extent))
    spot[longest] = (spot[longest] + 1) % extent[longest]
    return result.at[tuple(spot)].set(high)


def block_scale(stream_key, extent, pieces, smallest, largest):
    def one(dim, parts):
        steps = jax.random.uniform(jax.random.fold_in(jax.random.fold_in(stream_key, 6), dim), (parts,), jnp.float32, smallest / len(pieces), largest / len(pieces))
        return jnp.repeat(jnp.exp(steps), extent[dim] // parts).reshape((-1,) + (1,) * (len(extent) - dim - 1))

    loudness = one(*pieces[0])
    for cut in pieces[1:]:
        loudness = loudness * one(*cut)
    return loudness


def scatter_about(key, shape, scale, most, cuts=(), kind=jnp.bfloat16):
    level = block_scale(key, shape, cuts, -0.22, 0.18) if cuts else 1.0
    drawn = jax.random.normal(key, shape, jnp.float32) * scale * level
    return jnp.minimum(jnp.maximum(drawn, -most), most).astype(kind)


def setup_inputs(seed: int = 0) -> dict:
    splits = jax.random.split(jax.random.key(seed), 8)
    return {
        "velocity": scatter_about(splits[0], (3, NEX, NEY, EZ, NODES), 1.0, 6.0, ((1, 32), (2, 4))),
        "part_pos": jnp.clip(jax.random.uniform(splits[1], (NB, 3, SLOTS), jnp.float32, -1.0, 1.0) * block_scale(splits[1], (NB, 3, SLOTS), ((0, 128),), -0.4, 0.0), -1.0, 1.0),
        "part_vel": scatter_about(splits[2], (NB, 3, SLOTS), 1.0, 6.0, ((0, 128),), jnp.float32),
        "part_coef": jnp.clip(jnp.exp(math.log(3.0) - 2.3025851 * jax.random.uniform(splits[3], (NB, 2, SLOTS), jnp.float32) ** block_scale(splits[3], (NB, 2, SLOTS), ((0, 128),), -0.2, 0.2)), 0.3, 3.0),
        "counts": set_ends(jax.random.randint(splits[4], (NB,), 1, 129), jax.random.fold_in(splits[4], 1), 1, 128).astype(jnp.int32),
        "dest": draw_dest(jax.random.fold_in(splits[7], 71), 0),
        "elem": draw_elem(jax.random.fold_in(splits[7], 71), 0),
    }


GLL = (-1.0, -0.8717401485096066, -0.5917001814331423, -0.2092992179024789, 0.2092992179024789, 0.5917001814331423, 0.8717401485096066, 1.0)
HIGH = lax.Precision.HIGHEST
SHARPNESS = 8.0

def lagrange_rows(coord):
    layers = []
    for i in range(8):
        product = jnp.ones_like(coord)
        for m in range(8):
            if m != i:
                product = product * ((coord - GLL[m]) / (GLL[i] - GLL[m]))
        layers.append(product)
    return jnp.stack(layers, axis=1)

def gauss_rows(coord, offset):
    points = jnp.array(GLL, dtype=jnp.float32)
    spacing = points[None, :, None] - (coord[:, None, :] + offset)
    return jnp.exp(-SHARPNESS * spacing * spacing)

def element_step(field, position, carried, coefs, filled):
    group = field.shape[0]
    width = position.shape[2]
    basis_r = lagrange_rows(position[:, 0])
    basis_s = lagrange_rows(position[:, 1])
    basis_t = lagrange_rows(position[:, 2])
    nodal = field.reshape(group, 3, 8, 64)
    partial_sum = jnp.einsum('gcia,gip->gcap', nodal, basis_r, precision=HIGH)
    planes = (basis_s[:, :, None, :] * basis_t[:, None, :, :]).reshape(group, 64, width)
    fluid = lax.optimization_barrier(jnp.sum(partial_sum * planes[:, None], axis=2))
    relative = fluid - carried
    speed = jnp.sqrt(lax.optimization_barrier(jnp.sum(relative * relative, axis=1)))
    factor = coefs[:, 0] * (1.0 + 0.15 * jnp.power(coefs[:, 1] * speed, 0.687))
    live = jnp.arange(width, dtype=jnp.int32)[None, :] < filled[:, None]
    drag = jnp.where(live[:, None, :], factor[:, None, :] * relative, jnp.zeros_like(relative))
    weights_s = gauss_rows(position[:, 1], 0.0)
    weights_t = gauss_rows(position[:, 2], 0.0)
    spread = (-drag)[:, :, None, None, :] * weights_s[:, None, :, None, :] * weights_t[:, None, None, :, :]
    spread = spread.reshape(group, 192, width)
    weights_r = jnp.stack([gauss_rows(position[:, 0], 0.0), gauss_rows(position[:, 0], 2.0), gauss_rows(position[:, 0], -2.0)], axis=1)
    deposit = jnp.einsum('gsip,gap->gsia', weights_r, spread, precision=HIGH)
    deposit = deposit.reshape(group, 3, 8, 3, 64).transpose(0, 1, 3, 2, 4).reshape(group, 3, 3, 512)
    return (drag, deposit)

def run_groups(field, position, carried, coefs, filled, group):
    total = field.shape[0]
    turns = total // group
    packed = tuple((a.reshape((turns, group) + a.shape[1:]) for a in (field, position, carried, coefs, filled)))
    drag, deposit = lax.map(lambda args: element_step(*args), packed)
    return (drag.reshape((total,) + drag.shape[2:]), deposit.reshape((total,) + deposit.shape[2:]))

def dss_axis(field, elem_axis, node_axis, far_lo, far_hi):
    count = field.shape[elem_axis]
    lower = lax.slice_in_dim(field, 0, 1, axis=node_axis)
    upper = lax.slice_in_dim(field, 7, 8, axis=node_axis)
    edge_shape = lax.slice_in_dim(lower, 0, 1, axis=elem_axis).shape
    lower_next = jnp.concatenate([lax.slice_in_dim(lower, 1, count, axis=elem_axis), far_lo.reshape(edge_shape)], axis=elem_axis)
    upper_prev = jnp.concatenate([far_hi.reshape(edge_shape), lax.slice_in_dim(upper, 0, count - 1, axis=elem_axis)], axis=elem_axis)
    middle = lax.slice_in_dim(field, 1, 7, axis=node_axis)
    return jnp.concatenate([lower + upper_prev, middle, upper + lower_next], axis=node_axis)

def edge_zeros(field, elem_axis, node_axis):
    edge = lax.slice_in_dim(lax.slice_in_dim(field, 0, 1, axis=elem_axis), 0, 1, axis=node_axis)
    return jnp.zeros_like(edge).reshape(-1)

def reference(velocity, part_pos, part_vel, part_coef, counts, dest, elem):
    blocks = part_pos.shape[0]
    source_row = jnp.arange(blocks, dtype=jnp.int32) // (E_DEV * N_GY)
    local_x = elem // (EYD * EZ)
    local_y = elem // EZ % EYD
    local_z = elem % EZ
    global_id = ((source_row * EXD + local_x) * NEY + dest * EYD + local_y) * EZ + local_z
    by_elem = jnp.argsort(global_id)
    field_e = velocity.reshape(3, blocks, NODES).transpose(1, 0, 2).astype(jnp.float32)
    drag_e, deposit = run_groups(field_e, part_pos[by_elem], part_vel[by_elem], part_coef[by_elem], counts[by_elem], math.gcd(blocks, 256))
    drag = drag_e[global_id]
    deposit = deposit.transpose(1, 2, 0, 3).reshape(3, 3, NEX, NEY, EZ, 8, 8, 8)
    own_part, minus_part, plus_part = (deposit[0], deposit[1], deposit[2])
    empty_layer = jnp.zeros_like(own_part[:, 0:1])
    total = own_part + jnp.concatenate([minus_part[:, 1:], empty_layer], axis=1) + jnp.concatenate([empty_layer, plus_part[:, :-1]], axis=1)
    field = total
    for elem_axis, node_axis in ((1, 4), (2, 5), (3, 6)):
        zeros_edge = edge_zeros(field, elem_axis, node_axis)
        field = dss_axis(field, elem_axis, node_axis, zeros_edge, zeros_edge)
    return (drag, field.reshape(3, NEX, NEY, EZ, NODES))
```

```python
import jax
import jax.numpy as jnp
import numpy as np
from jax import lax
from jax.experimental import pallas as pl
from jax.experimental.pallas import tpu as pltpu
from jax.sharding import PartitionSpec as P

GLL = (
    -1.0,
    -0.8717401485096066,
    -0.5917001814331423,
    -0.2092992179024789,
    0.2092992179024789,
    0.5917001814331423,
    0.8717401485096066,
    1.0,
)
SHARPNESS = 8.0
INTERPRET = False
F32 = jnp.float32
BF16 = jnp.bfloat16
VMEM = pltpu.VMEM
SMEM = pltpu.SMEM
N_GY = 4
SHARE = 32
ROWS = 264
PAIRED = (0, 2, 4, 6, 1, 3, 5, 7)


def node_table():
    q = np.array(GLL, np.float64)
    rows = []
    for order in (tuple(range(8)), PAIRED):
        for t in range(7):
            rows.append([q[[m for m in range(8) if m != i][t]] for i in order])
        rows.append([1.0 / np.prod([q[i] - q[m] for m in range(8) if m != i]) for i in order])
    rows.append([q[i] for i in range(8)])
    for shift in (-2.0, 0.0, 2.0):
        rows.append([q[i] + shift for i in PAIRED])
    table = np.array(rows, np.float32).reshape(-1, 1)
    return np.ascontiguousarray(np.broadcast_to(table, (table.shape[0], 128)))


NODE_ROWS = 8 * 20


def whole(space=VMEM):
    return pl.BlockSpec(memory_space=space)


def call(kernel, out_shape, out_specs, in_specs, scratch=()):
    return pl.pallas_call(
        kernel,
        out_shape=out_shape,
        in_specs=in_specs,
        out_specs=out_specs,
        scratch_shapes=scratch,
        interpret=INTERPRET,
    )


def lanes(shape=(1, 128)):
    return lax.broadcasted_iota(jnp.int32, shape, len(shape) - 1)


def pack_kernel(dest, counts, elem, pos, vel, coef, send, slot):
    lane = lanes()
    ids = lax.broadcasted_iota(jnp.int32, (8, 128), 0) * 128 + lanes((8, 128))

    def one(b, state):
        taken, labels = state
        d = dest[b]
        r = (taken >> (8 * d)) & 255
        slot[b] = d * 96 + r
        base = d * ROWS + r
        send[pl.ds(base, 3, stride=32), :] = pos[pl.ds(b, 3, stride=128), :]
        send[pl.ds(base + 96, 3, stride=32), :] = vel[pl.ds(b, 3, stride=128), :]
        rate = coef[pl.ds(2 * b, 1), :]
        send[pl.ds(base + 192, 1), :] = jnp.where(lane < counts[b], rate, 0.0)
        send[pl.ds(base + 224, 1), :] = coef[pl.ds(2 * b + 1, 1), :]
        labels = jnp.where(ids == d * 128 + r, elem[b], labels)
        return (taken + (1 << (8 * d)), labels)

    _, labels = lax.fori_loop(0, 128, one, (jnp.int32(0), jnp.zeros((8, 128), jnp.int32)), unroll=8)
    labels = labels.astype(F32)
    for d in range(N_GY):
        send[d * ROWS + 256 : d * ROWS + 264, :] = jnp.broadcast_to(labels[d : d + 1, :], (8, 128))


def split_two(x):
    high = x.astype(BF16)
    low = (x - high.astype(F32)).astype(BF16)
    return high, low


def lagrange(x, nodes, first):
    out = nodes[8 * (first + 7) : 8 * (first + 8), :]
    for t in range(7):
        out = out * (x - nodes[8 * (first + t) : 8 * (first + t + 1), :])
    return out


def gauss(x, nodes, row):
    d = nodes[8 * row : 8 * row + 8, :] - x
    return jnp.exp(d * d * (-SHARPNESS))


def outer(a, b):
    return jnp.concatenate([a[j : j + 1, :] * b for j in range(8)], axis=0)


def main_kernel(
    recv, vel, nodes, drag, inside, ghost_lo, ghost_hi, field, fluid, parts, lab_v, lab_s, sem
):
    low_half = lanes((1, 128)) < 64
    for s in range(N_GY):
        lab_v[s : s + 1, :] = recv[s * ROWS + 256 : s * ROWS + 257, :].astype(jnp.int32)
    copy = pltpu.make_async_copy(lab_v, lab_s, sem)
    copy.start()

    def spread_field(xy, _):
        for c in range(3):
            for h in range(4):
                t = vel[c * 8 + xy, :, 128 * h : 128 * h + 128].astype(F32)
                turned = pltpu.roll(t, 64, 1)
                at = xy * 384 + (c * 8 + h) * 16
                field[pl.ds(at, 16), :] = jnp.where(low_half, t, turned)
                field[pl.ds(at + 64, 16), :] = jnp.where(low_half, turned, t)
        return 0

    lax.fori_loop(0, 8, spread_field, 0)
    copy.wait()

    def interpolate(n, _):
        s = n // SHARE
        r = n % SHARE
        e = lab_s[s, r]
        xy = e // 16
        z = e % 16
        base = s * ROWS + r
        basis_r = lagrange(recv[pl.ds(base, 1), :], nodes, 8)
        basis_s = lagrange(recv[pl.ds(base + 32, 1), :], nodes, 0)
        basis_t = lagrange(recv[pl.ds(base + 64, 1), :], nodes, 0)
        high, low = split_two(outer(basis_s, basis_t))
        nodal = field[pl.ds(xy * 384 + z, 24, stride=16), :].astype(BF16)
        part = jnp.dot(nodal, jnp.concatenate([high, low], axis=0), preferred_element_type=F32)
        for c in range(3):
            fluid[pl.ds(s * 96 + c * 32 + r, 1), :] = jnp.sum(
                part[8 * c : 8 * c + 8, :] * basis_r, axis=0, keepdims=True
            )
        return 0

    lax.fori_loop(0, 128, interpolate, 0, unroll=8)

    for s in range(N_GY):
        w = [
            fluid[s * 96 + 32 * c : s * 96 + 32 * c + 32, :]
            - recv[s * ROWS + 96 + 32 * c : s * ROWS + 128 + 32 * c, :]
            for c in range(3)
        ]
        rate = recv[s * ROWS + 192 : s * ROWS + 224, :]
        scale = recv[s * ROWS + 224 : s * ROWS + 256, :]
        square = (w[0] * w[0] + w[1] * w[1] + w[2] * w[2]) * (scale * scale)
        power = jnp.where(square > 0.0, jnp.exp(0.3435 * jnp.log(square)), 0.0)
        factor = rate * (1.0 + 0.15 * power)
        for c in range(3):
            drag[s * 96 + 32 * c : s * 96 + 32 * c + 32, :] = factor * w[c]

    def project(n, _):
        s = n // SHARE
        r = n % SHARE
        e = lab_s[s, r]
        xy = e // 16
        z = e % 16
        base = s * ROWS + r
        x = recv[pl.ds(base, 1), :]
        weights = [gauss(x, nodes, 17 + k) for k in range(3)]
        planes = outer(
            gauss(recv[pl.ds(base + 32, 1), :], nodes, 16),
            gauss(recv[pl.ds(base + 64, 1), :], nodes, 16),
        )
        planes = jnp.concatenate(split_two(planes), axis=0)
        rows = []
        for c in range(3):
            force = -drag[pl.ds(s * 96 + c * 32 + r, 1), :]
            rows += [wr * force for wr in weights]
        rows = jnp.concatenate(split_two(jnp.concatenate(rows, axis=0)), axis=0)
        both = lax.dot_general(
            rows, planes, (((1,), (1,)), ((), ())), preferred_element_type=F32
        )
        both = both[:72, :] + both[72:, :]
        both = both + pltpu.roll(both, 64, 1)
        for k in range(9):
            t = both[8 * k : 8 * k + 8, :]
            t = jnp.where(low_half, t, pltpu.roll(t, 4, 0))
            parts[pl.ds(xy * 576 + k * 64 + z, 4, stride=16), :] = t[0:4, :]
        return 0

    lax.fori_loop(0, 128, project, 0, unroll=4)

    def part(x, y, c, k, h):
        return parts[pl.ds((x * 4 + y) * 576 + (c * 3 + k) * 64 + h * 16, 16), :]

    def gather_parts(y, _):
        for c in range(3):
            lower = []
            upper = []
            for h in range(4):
                lo = part(0, y, c, 1, h) + part(1, y, c, 0, h)
                hi = part(1, y, c, 1, h) + part(0, y, c, 2, h)
                inside[c * 8 + y, :, 128 * h : 128 * h + 128] = lo
                inside[c * 8 + 4 + y, :, 128 * h : 128 * h + 128] = hi
                lower.append(lo)
                upper.append(hi)
            for h in range(4):
                lo = part(0, y, c, 0, h)
                hi = part(1, y, c, 2, h)
                if h == 3:
                    lo = lo + jnp.where(low_half, 0.0, pltpu.roll(lower[0], 64, 1))
                if h == 0:
                    hi = hi + jnp.where(low_half, pltpu.roll(upper[3], 64, 1), 0.0)
                ghost_lo[c * 4 + y, :, 128 * h : 128 * h + 128] = lo
                ghost_hi[c * 4 + y, :, 128 * h : 128 * h + 128] = hi
        return 0

    lax.fori_loop(0, 4, gather_parts, 0)


def first_pass_kernel(ends, inside, sent_lo, sent_hi, got_lo, got_hi, field, face_lo, face_hi):
    low_half = lanes((1, 128)) < 64
    spot = (lanes((1, 128)) % 64) // 8
    has_before = ends[0] > 0
    has_after = ends[1] > 0

    def cut(ref, at, h):
        return ref[at, :, 128 * h : 128 * h + 128]

    for c in range(3):
        packed = [jnp.zeros((16, 128), F32), jnp.zeros((16, 128), F32)]
        for y in range(4):
            lower = [cut(inside, c * 8 + y, h) + cut(got_lo, c * 4 + y, h) for h in range(4)]
            upper = [cut(inside, c * 8 + 4 + y, h) + cut(got_hi, c * 4 + y, h) for h in range(4)]
            first = cut(got_lo, c * 4 + y, 0) + pltpu.roll(cut(sent_lo, c * 4 + y, 3), 64, 1)
            last = cut(got_hi, c * 4 + y, 3) + pltpu.roll(cut(sent_hi, c * 4 + y, 0), 64, 1)
            low3, up0 = lower[3], upper[0]
            lower[0] = jnp.where(low_half & has_before, first, lower[0])
            upper[3] = jnp.where(low_half | jnp.logical_not(has_after), upper[3], last)
            lower[3] = jnp.where(low_half, low3, low3 + pltpu.roll(up0, 64, 1))
            upper[0] = jnp.where(low_half, up0 + pltpu.roll(low3, 64, 1), up0)
            for x, layer in ((0, lower), (1, upper)):
                for h in range(4):
                    field[c * 8 + x * 4 + y, :, 128 * h : 128 * h + 128] = layer[h]
                    k = x * 4 + h
                    if y == 0:
                        moved = pltpu.roll(layer[h], 8 * k, 1) if k else layer[h]
                        packed[0] = jnp.where(spot == k, moved, packed[0])
                    if y == 3:
                        by = (8 * k - 56) % 128
                        moved = pltpu.roll(layer[h], by, 1) if by else layer[h]
                        packed[1] = jnp.where(spot == k, moved, packed[1])
        face_lo[16 * c : 16 * c + 16, :] = packed[0]
        face_hi[16 * c : 16 * c + 16, :] = packed[1]


def last_pass_kernel(field, got_lo, got_hi, ret, slot, out, drag):
    lane = lanes((1, 128))
    bottom = (lane % 64) < 8
    top = (lane % 64) >= 56
    z = lax.broadcasted_iota(jnp.int32, (16, 128), 0)
    lane16 = lanes((16, 128))
    up_here = (lane16 % 8 == 7) & (z < 15)
    down_here = (lane16 % 8 == 0) & (z > 0)

    def one_comp(c, _):
        lo_pack = got_lo[pl.ds(16 * c, 16), :]
        hi_pack = got_hi[pl.ds(16 * c, 16), :]
        for x in range(2):
            for h in range(4):
                k = x * 4 + h
                f = [field[c * 8 + x * 4 + y, :, 128 * h : 128 * h + 128] for y in range(4)]
                down = lo_pack if k == 0 else pltpu.roll(lo_pack, (128 - 8 * k) % 128, 1)
                up = hi_pack if k == 7 else pltpu.roll(hi_pack, 56 - 8 * k, 1)
                for y in range(4):
                    above = up if y == 3 else pltpu.roll(f[y + 1], 56, 1)
                    below = down if y == 0 else pltpu.roll(f[y - 1], 72, 1)
                    g = f[y] + jnp.where(top, above, jnp.where(bottom, below, 0.0))
                    above = pltpu.roll(pltpu.roll(g, 7, 1), 15, 0)
                    below = pltpu.roll(pltpu.roll(g, 121, 1), 1, 0)
                    g = g + jnp.where(up_here, above, jnp.where(down_here, below, 0.0))
                    out[c * 8 + x * 4 + y, :, 128 * h : 128 * h + 128] = g
        return 0

    lax.fori_loop(0, 3, one_comp, 0)

    def unpack(b, _):
        drag[pl.ds(b, 3, stride=128), :] = ret[pl.ds(slot[b], 3, stride=32), :]
        return 0

    lax.fori_loop(0, 128, unpack, 0, unroll=8)


def shifted(shard, axis, by):
    count = lax.axis_size(axis)
    pairs = [(i, i + by) for i in range(count) if 0 <= i + by < count]
    return lax.ppermute(shard, axis, pairs)


def sds(*shape, dtype=F32):
    return jax.ShapeDtypeStruct(shape, dtype)


def body(velocity, part_pos, part_vel, part_coef, counts, dest, elem):
    pos = part_pos.transpose(1, 0, 2).reshape(384, 128)
    vel = part_vel.transpose(1, 0, 2).reshape(384, 128)
    coef = part_coef.reshape(256, 128)
    nodes = jnp.asarray(node_table())
    send, slot = call(
        pack_kernel,
        (sds(N_GY * ROWS, 128), sds(128, dtype=jnp.int32)),
        (whole(), whole(SMEM)),
        [whole(SMEM)] * 3 + [whole()] * 3,
    )(dest, counts, elem, pos, vel, coef)
    recv = lax.all_to_all(
        send.reshape(N_GY, ROWS, 128), "gy", split_axis=0, concat_axis=0, tiled=True
    ).reshape(N_GY * ROWS, 128)
    drag_e, inside, ghost_lo, ghost_hi = call(
        main_kernel,
        (sds(384, 128), sds(24, 16, 512), sds(12, 16, 512), sds(12, 16, 512)),
        (whole(),) * 4,
        [whole()] * 3,
        (
            VMEM((8 * 384, 128), F32),
            VMEM((384, 128), F32),
            VMEM((8 * 576, 128), F32),
            VMEM((8, 128), jnp.int32),
            SMEM((8, 128), jnp.int32),
            pltpu.SemaphoreType.DMA,
        ),
    )(recv, velocity.reshape(24, 16, 512), nodes)
    got_hi = shifted(ghost_lo, "gx", -1)
    got_lo = shifted(ghost_hi, "gx", 1)
    ret = lax.all_to_all(
        drag_e.reshape(N_GY, 96, 128), "gy", split_axis=0, concat_axis=0, tiled=True
    ).reshape(384, 128)
    at = lax.axis_index("gx")
    ends = jnp.stack([at, lax.axis_size("gx") - 1 - at]).astype(jnp.int32)
    field, face_lo, face_hi = call(
        first_pass_kernel,
        (sds(24, 16, 512), sds(48, 128), sds(48, 128)),
        (whole(),) * 3,
        [whole(SMEM)] + [whole()] * 5,
    )(ends, inside, ghost_lo, ghost_hi, got_lo, got_hi)
    face_after = shifted(face_lo, "gy", -1)
    face_before = shifted(face_hi, "gy", 1)
    out, drag = call(
        last_pass_kernel,
        (sds(24, 16, 512), sds(384, 128)),
        (whole(), whole()),
        [whole()] * 4 + [whole(SMEM)],
    )(field, face_before, face_after, ret, slot)
    return (
        drag.reshape(3, 128, 128).transpose(1, 0, 2),
        out.reshape(velocity.shape),
    )


def solution(mesh):
    in_specs = (
        P(None, "gx", "gy", None, None),
        P(("gx", "gy"), None, None),
        P(("gx", "gy"), None, None),
        P(("gx", "gy"), None, None),
        P(("gx", "gy")),
        P(("gx", "gy")),
        P(("gx", "gy")),
    )
    out_specs = (P(("gx", "gy"), None, None), P(None, "gx", "gy", None, None))
    return jax.shard_map(body, mesh=mesh, in_specs=in_specs, out_specs=out_specs, check_vma=False)
```

```python
import jax
import jax.numpy as jnp
import numpy as np
from jax import lax
from jax.experimental import pallas as pl
from jax.experimental.pallas import tpu as pltpu
from jax.sharding import PartitionSpec as P

GLL = (
    -1.0,
    -0.8717401485096066,
    -0.5917001814331423,
    -0.2092992179024789,
    0.2092992179024789,
    0.5917001814331423,
    0.8717401485096066,
    1.0,
)
SHARPNESS = 8.0
INTERPRET = False
F32 = jnp.float32
BF16 = jnp.bfloat16
VMEM = pltpu.VMEM
SMEM = pltpu.SMEM
N_GY = 4
SHARE = 32
ROWS = 264
PAIRED = (0, 2, 4, 6, 1, 3, 5, 7)


def node_table():
    q = np.array(GLL, np.float64)
    rows = []
    for order in (tuple(range(8)), PAIRED):
        for t in range(7):
            rows.append([q[[m for m in range(8) if m != i][t]] for i in order])
        rows.append([1.0 / np.prod([q[i] - q[m] for m in range(8) if m != i]) for i in order])
    rows.append([q[i] for i in range(8)])
    for shift in (-2.0, 0.0, 2.0):
        rows.append([q[i] + shift for i in PAIRED])
    table = np.array(rows, np.float32).reshape(-1, 1)
    return np.ascontiguousarray(np.broadcast_to(table, (table.shape[0], 128)))


UNROLL_A = 16
UNROLL_B = 8
OWN_FLOPS = 2_000_000_000
UNPACK_FLOPS = 1_000_000_000


def call(kernel, outs, ins, scratch=(), flops=0, aliases=None):
    args = [
        a
        if INTERPRET
        else pltpu.with_memory_space_constraint(a, VMEM if m == "vmem" else pltpu.HBM)
        if m in ("vmem", "hbm", "table")
        else a
        for a, m in ins
    ]
    shapes = [
        VMEM(shape, dtype) if m == "vmem" and not INTERPRET else jax.ShapeDtypeStruct(shape, dtype)
        for shape, dtype, m in outs
    ]
    return pl.pallas_call(
        kernel,
        out_shape=shapes,
        in_specs=[pl.BlockSpec(memory_space=SMEM if m in ("smem", "table") else VMEM) for _, m in ins],
        out_specs=[pl.BlockSpec(memory_space=SMEM if m == "smem" else VMEM) for _, _, m in outs],
        scratch_shapes=scratch,
        interpret=INTERPRET,
        input_output_aliases=aliases or {},
        compiler_params=pltpu.CompilerParams(vmem_limit_bytes=24 * 1024 * 1024),
        cost_estimate=pl.CostEstimate(flops=flops, bytes_accessed=0, transcendentals=0),
    )(*args)


def lanes(shape=(1, 128)):
    return lax.broadcasted_iota(jnp.int32, shape, len(shape) - 1)


def pack_kernel(dest, counts, elem, pos, vel, coef, send, block, own_elem):
    me = lax.axis_index("gy")
    lane = lanes()
    ids = lax.broadcasted_iota(jnp.int32, (8, 128), 0) * 128 + lanes((8, 128))

    def one(b, state):
        taken, labels = state
        d = dest[b] ^ me
        r = (taken >> (8 * d)) & 255
        block[d * SHARE + r] = b
        base = d * ROWS + r
        send[pl.ds(base, 3, stride=32), :] = pos[pl.ds(b, 3, stride=128), :]
        send[pl.ds(base + 96, 3, stride=32), :] = vel[pl.ds(b, 3, stride=128), :]
        rate = coef[pl.ds(2 * b, 1), :]
        send[pl.ds(base + 192, 1), :] = jnp.where(lane < counts[b], rate, 0.0)
        send[pl.ds(base + 224, 1), :] = coef[pl.ds(2 * b + 1, 1), :]
        own_elem[d * SHARE + r] = elem[b]
        labels = jnp.where(ids == d * 128 + r, elem[b], labels)
        return (taken + (1 << (8 * d)), labels)

    _, labels = lax.fori_loop(0, 128, one, (jnp.int32(0), jnp.zeros((8, 128), jnp.int32)), unroll=8)
    labels = labels.astype(F32)
    for d in range(N_GY):
        send[d * ROWS + 256 : d * ROWS + 264, :] = jnp.broadcast_to(labels[d : d + 1, :], (8, 128))


def split_two(x):
    high = x.astype(BF16)
    low = (x - high.astype(F32)).astype(BF16)
    return high, low


def lagrange(x, nodes, first):
    out = nodes[8 * (first + 7) : 8 * (first + 8), :]
    for t in range(7):
        out = out * (x - nodes[8 * (first + t) : 8 * (first + t + 1), :])
    return out


def gauss(x, nodes, row):
    d = nodes[8 * row : 8 * row + 8, :] - x
    return jnp.exp(d * d * (-SHARPNESS))


def outer(a, b):
    return jnp.concatenate([a[j : j + 1, :] * b for j in range(8)], axis=0)


def spread_field(vel, field):
    low_half = lanes() < 64

    def one(xy, _):
        for c in range(3):
            for h in range(4):
                t = vel[c * 8 + xy, :, 128 * h : 128 * h + 128].astype(F32)
                turned = pltpu.roll(t, 64, 1)
                at = xy * 384 + (c * 8 + h) * 16
                field[pl.ds(at, 16), :] = jnp.where(low_half, t, turned)
                field[pl.ds(at + 64, 16), :] = jnp.where(low_half, turned, t)
        return 0

    lax.fori_loop(0, 8, one, 0)


def interpolate(group, element, field, nodes, fluid):
    def one(r, _):
        e = element(r)
        basis_r = lagrange(group[pl.ds(r, 1), :], nodes, 8)
        basis_s = lagrange(group[pl.ds(r + 32, 1), :], nodes, 0)
        basis_t = lagrange(group[pl.ds(r + 64, 1), :], nodes, 0)
        high, low = split_two(outer(basis_s, basis_t))
        nodal = field[pl.ds((e >> 4) * 384 + (e & 15), 24, stride=16), :].astype(BF16)
        part = jnp.dot(nodal, jnp.concatenate([high, low], axis=0), preferred_element_type=F32)
        for c in range(3):
            fluid[pl.ds(c * 32 + r, 1), :] = jnp.sum(
                part[8 * c : 8 * c + 8, :] * basis_r, axis=0, keepdims=True
            )
        return 0

    lax.fori_loop(0, SHARE, one, 0, unroll=UNROLL_A)


def find_drag(group, fluid, drag):
    w = [
        fluid[32 * c : 32 * c + 32, :] - group[96 + 32 * c : 128 + 32 * c, :] for c in range(3)
    ]
    scale = group[224:256, :]
    square = (w[0] * w[0] + w[1] * w[1] + w[2] * w[2]) * (scale * scale)
    power = jnp.where(square > 0.0, jnp.exp(0.3435 * jnp.log(square)), 0.0)
    factor = group[192:224, :] * (1.0 + 0.15 * power)
    for c in range(3):
        drag[32 * c : 32 * c + 32, :] = factor * w[c]


def project(group, element, drag, nodes, parts):
    low_half = lanes() < 64

    def one(r, _):
        e = element(r)
        x = group[pl.ds(r, 1), :]
        weights = [gauss(x, nodes, 17 + k) for k in range(3)]
        planes = outer(
            gauss(group[pl.ds(r + 32, 1), :], nodes, 16),
            gauss(group[pl.ds(r + 64, 1), :], nodes, 16),
        )
        planes = jnp.concatenate(split_two(planes), axis=0)
        rows = []
        for c in range(3):
            force = -drag[pl.ds(c * 32 + r, 1), :]
            rows += [wr * force for wr in weights]
        rows = jnp.concatenate(split_two(jnp.concatenate(rows, axis=0)), axis=0)
        both = lax.dot_general(
            rows, planes, (((1,), (1,)), ((), ())), preferred_element_type=F32
        )
        both = both[:72, :] + both[72:, :]
        both = both + pltpu.roll(both, 64, 1)
        at = (e >> 4) * 576 + (e & 15)
        for k in range(9):
            t = both[8 * k : 8 * k + 8, :]
            t = jnp.where(low_half, t, pltpu.roll(t, 4, 0))
            parts[pl.ds(at + k * 64, 4, stride=16), :] = t[0:4, :]
        return 0

    lax.fori_loop(0, SHARE, one, 0, unroll=UNROLL_B)


def own_kernel(elem, group, vel, nodes, field, parts, drag, fluid):
    def element(r):
        return elem[r]

    spread_field(vel, field)
    interpolate(group, element, field, nodes, fluid)
    find_drag(group, fluid, drag)
    project(group, element, drag, nodes, parts)


def rest_kernel(
    g1, g2, g3, field, nodes, _, d1, d2, d3, inside, ghosts, parts, fluid, lab_v, lab_s, sem
):
    groups = (g1, g2, g3)
    drags = (d1, d2, d3)
    for k, g in enumerate(groups):
        lab_v[k : k + 1, :] = g[256:257, :].astype(jnp.int32)
    copy = pltpu.make_async_copy(lab_v, lab_s, sem)
    copy.start()
    copy.wait()
    elements = [lambda r, k=k: lab_s[k, r] for k in range(3)]
    for k in range(3):
        interpolate(groups[k], elements[k], field, nodes, fluid)
        find_drag(groups[k], fluid, drags[k])
    for k in range(3):
        project(groups[k], elements[k], drags[k], nodes, parts)
    gather_parts(parts, inside, ghosts)


def gather_parts(parts, inside, ghosts):
    low_half = lanes() < 64
    odd = lax.axis_index("gx") & 1
    to_lo = (1 - odd) * 12
    to_hi = odd * 12

    def part(x, y, c, k, h):
        return parts[pl.ds((x * 4 + y) * 576 + (c * 3 + k) * 64 + h * 16, 16), :]

    def one(y, _):
        for c in range(3):
            lower = []
            upper = []
            for h in range(4):
                lo = part(0, y, c, 1, h) + part(1, y, c, 0, h)
                hi = part(1, y, c, 1, h) + part(0, y, c, 2, h)
                inside[c * 8 + y, :, 128 * h : 128 * h + 128] = lo
                inside[c * 8 + 4 + y, :, 128 * h : 128 * h + 128] = hi
                lower.append(lo)
                upper.append(hi)
            for h in range(4):
                lo = part(0, y, c, 0, h)
                hi = part(1, y, c, 2, h)
                if h == 3:
                    lo = lo + jnp.where(low_half, 0.0, pltpu.roll(lower[0], 64, 1))
                if h == 0:
                    hi = hi + jnp.where(low_half, pltpu.roll(upper[3], 64, 1), 0.0)
                ghosts[to_lo + c * 4 + y, :, 128 * h : 128 * h + 128] = lo
                ghosts[to_hi + c * 4 + y, :, 128 * h : 128 * h + 128] = hi
        return 0

    lax.fori_loop(0, 4, one, 0)


def first_pass_kernel(last_gx, inside, sent, near, far, field, faces):
    low_half = lanes() < 64
    spot = (lanes() % 64) // 8
    gx = lax.axis_index("gx")
    odd = (gx & 1) == 1
    has_before = gx > 0
    has_after = gx < last_gx
    to_lo = (1 - (gx & 1)) * 12
    to_hi = (gx & 1) * 12
    y_odd = (lax.axis_index("gy") & 1) == 1

    def cut(ref, at, h):
        return ref[at, :, 128 * h : 128 * h + 128]

    for c in range(3):
        packed = [jnp.zeros((16, 128), F32), jnp.zeros((16, 128), F32)]
        for y in range(4):
            pair = [(cut(near, c * 4 + y, h), cut(far, c * 4 + y, h)) for h in range(4)]
            got_lo = [jnp.where(odd, n, f) for n, f in pair]
            got_hi = [jnp.where(odd, f, n) for n, f in pair]
            lower = [cut(inside, c * 8 + y, h) + got_lo[h] for h in range(4)]
            upper = [cut(inside, c * 8 + 4 + y, h) + got_hi[h] for h in range(4)]
            first = got_lo[0] + pltpu.roll(cut(sent, to_lo + c * 4 + y, 3), 64, 1)
            last = got_hi[3] + pltpu.roll(cut(sent, to_hi + c * 4 + y, 0), 64, 1)
            low3, up0 = lower[3], upper[0]
            lower[0] = jnp.where(low_half & has_before, first, lower[0])
            upper[3] = jnp.where(low_half | jnp.logical_not(has_after), upper[3], last)
            lower[3] = jnp.where(low_half, low3, low3 + pltpu.roll(up0, 64, 1))
            upper[0] = jnp.where(low_half, up0 + pltpu.roll(low3, 64, 1), up0)
            for x, layer in ((0, lower), (1, upper)):
                for h in range(4):
                    field[c * 8 + x * 4 + y, :, 128 * h : 128 * h + 128] = layer[h]
                    k = x * 4 + h
                    if y == 0:
                        moved = pltpu.roll(layer[h], 8 * k, 1) if k else layer[h]
                        packed[0] = jnp.where(spot == k, moved, packed[0])
                    if y == 3:
                        by = (8 * k - 56) % 128
                        moved = pltpu.roll(layer[h], by, 1) if by else layer[h]
                        packed[1] = jnp.where(spot == k, moved, packed[1])
        faces[16 * c : 16 * c + 16, :] = jnp.where(y_odd, packed[0], packed[1])
        faces[48 + 16 * c : 64 + 16 * c, :] = jnp.where(y_odd, packed[1], packed[0])


def last_pass_kernel(field, got1, got3, out):
    lane = lanes()
    bottom = (lane % 64) < 8
    top = (lane % 64) >= 56
    z = lax.broadcasted_iota(jnp.int32, (16, 128), 0)
    lane16 = lanes((16, 128))
    up_here = (lane16 % 8 == 7) & (z < 15)
    down_here = (lane16 % 8 == 0) & (z > 0)
    odd = (lax.axis_index("gy") & 1) == 1

    def one_comp(c, _):
        one = got1[pl.ds(16 * c, 16), :]
        three = got3[pl.ds(16 * c, 16), :]
        lo_pack = jnp.where(odd, one, three)
        hi_pack = jnp.where(odd, three, one)
        for x in range(2):
            for h in range(4):
                k = x * 4 + h
                f = [field[c * 8 + x * 4 + y, :, 128 * h : 128 * h + 128] for y in range(4)]
                down = lo_pack if k == 0 else pltpu.roll(lo_pack, (128 - 8 * k) % 128, 1)
                up = hi_pack if k == 7 else pltpu.roll(hi_pack, 56 - 8 * k, 1)
                for y in range(4):
                    above = up if y == 3 else pltpu.roll(f[y + 1], 56, 1)
                    below = down if y == 0 else pltpu.roll(f[y - 1], 72, 1)
                    g = f[y] + jnp.where(top, above, jnp.where(bottom, below, 0.0))
                    above = pltpu.roll(pltpu.roll(g, 7, 1), 15, 0)
                    below = pltpu.roll(pltpu.roll(g, 121, 1), 1, 0)
                    g = g + jnp.where(up_here, above, jnp.where(down_here, below, 0.0))
                    out[c * 8 + x * 4 + y, :, 128 * h : 128 * h + 128] = g
        return 0

    lax.fori_loop(0, 3, one_comp, 0)


def unpack_kernel(block, d0, d1, d2, d3, drag):
    for k, d in enumerate((d0, d1, d2, d3)):

        def one(r, _):
            drag[pl.ds(block[k * SHARE + r], 3, stride=128), :] = d[pl.ds(r, 3, stride=32), :]
            return 0

        lax.fori_loop(0, SHARE, one, 0, unroll=8)


def swapped(x, axis, partner):
    count = lax.axis_size(axis)
    pairs = [(i, partner(i)) for i in range(count) if 0 <= partner(i) < count]
    return lax.ppermute(x, axis, pairs)


def body(velocity, part_pos, part_vel, part_coef, counts, dest, elem):
    pos = part_pos.transpose(1, 0, 2).reshape(384, 128)
    vel = part_vel.transpose(1, 0, 2).reshape(384, 128)
    coef = part_coef.reshape(256, 128)
    nodes = jnp.asarray(node_table())
    send, block, own_elem = call(
        pack_kernel,
        [((N_GY * ROWS, 128), F32, "vmem"), ((128,), jnp.int32, "smem"), ((128,), jnp.int32, "smem")],
        [(dest, "table"), (counts, "table"), (elem, "table"), (pos, "hbm"), (vel, "hbm"), (coef, "hbm")],
    )
    own = send[:ROWS]
    groups = [
        swapped(send[k * ROWS : (k + 1) * ROWS], "gy", lambda i, k=k: i ^ k) for k in range(1, N_GY)
    ]
    field, parts, drag_own = call(
        own_kernel,
        [((8 * 384, 128), F32, "vmem"), ((8 * 576, 128), F32, "vmem"), ((96, 128), F32, "vmem")],
        [(own_elem, "smem"), (own, "vmem"), (velocity.reshape(24, 16, 512), "hbm"), (nodes, "")],
        (VMEM((96, 128), F32),),
        flops=OWN_FLOPS,
    )
    *drags, inside, ghosts, _ = call(
        rest_kernel,
        [((96, 128), F32, "vmem")] * 3
        + [((24, 16, 512), F32, "vmem")] * 2
        + [((8 * 576, 128), F32, "vmem")],
        [(g, "vmem") for g in groups] + [(field, "vmem"), (nodes, ""), (parts, "vmem")],
        (
            VMEM((96, 128), F32),
            VMEM((8, 128), jnp.int32),
            SMEM((8, 128), jnp.int32),
            pltpu.SemaphoreType.DMA,
        ),
        aliases={5: 5},
    )
    far = swapped(ghosts[12:], "gx", lambda i: i + 1 if i & 1 else i - 1)
    near = swapped(ghosts[:12], "gx", lambda i: i ^ 1)
    back = [swapped(d, "gy", lambda i, k=k: i ^ k) for k, d in enumerate(drags, 1)]
    last_gx = lax.axis_size("gx") - 1
    field, faces = call(
        lambda *refs: first_pass_kernel(last_gx, *refs),
        [((24, 16, 512), F32, "vmem"), ((96, 128), F32, "vmem")],
        [(inside, "vmem"), (ghosts, "vmem"), (near, "vmem"), (far, "vmem")],
    )
    got1 = swapped(faces[:48], "gy", lambda i: i ^ 1)
    got3 = lax.ppermute(faces[48:], "gy", [(1, 2), (2, 1)])
    (drag,) = call(
        unpack_kernel,
        [((384, 128), F32, "")],
        [(block, "smem"), (drag_own, "vmem")] + [(d, "vmem") for d in back],
        flops=UNPACK_FLOPS,
    )
    (out,) = call(
        last_pass_kernel,
        [((24, 16, 512), F32, "")],
        [(field, "vmem"), (got1, "vmem"), (got3, "vmem")],
    )
    return (
        drag.reshape(3, 128, 128).transpose(1, 0, 2),
        out.reshape(velocity.shape),
    )


def solution(mesh):
    in_specs = (
        P(None, "gx", "gy", None, None),
        P(("gx", "gy"), None, None),
        P(("gx", "gy"), None, None),
        P(("gx", "gy"), None, None),
        P(("gx", "gy")),
        P(("gx", "gy")),
        P(("gx", "gy")),
    )
    out_specs = (P(("gx", "gy"), None, None), P(None, "gx", "gy", None, None))
    return jax.shard_map(body, mesh=mesh, in_specs=in_specs, out_specs=out_specs, check_vma=False)
```

```python
import jax
import jax.numpy as jnp
import numpy as np
from jax import lax
from jax.experimental import pallas as pl
from jax.experimental.pallas import tpu as pltpu
from jax.sharding import PartitionSpec as P

GLL = (
    -1.0,
    -0.8717401485096066,
    -0.5917001814331423,
    -0.2092992179024789,
    0.2092992179024789,
    0.5917001814331423,
    0.8717401485096066,
    1.0,
)
SHARPNESS = 8.0
INTERPRET = False
F32 = jnp.float32
BF16 = jnp.bfloat16
VMEM = pltpu.VMEM
SMEM = pltpu.SMEM
N_GY = 4
SHARE = 32
ROWS = 264
PAIRED = (0, 2, 4, 6, 1, 3, 5, 7)


def node_table():
    q = np.array(GLL, np.float64)
    rows = []
    for order in (tuple(range(8)), PAIRED):
        for t in range(7):
            rows.append([q[[m for m in range(8) if m != i][t]] for i in order])
        rows.append([1.0 / np.prod([q[i] - q[m] for m in range(8) if m != i]) for i in order])
    rows.append([q[i] for i in range(8)])
    for first, second in ((-2.0, 0.0), (2.0, 2.0)):
        for half in (PAIRED[:4], PAIRED[4:]):
            rows.append([q[i] + first for i in half] + [q[i] + second for i in half])
    table = np.array(rows, np.float32).reshape(-1, 1)
    return np.ascontiguousarray(np.broadcast_to(table, (table.shape[0], 128)))


PITCH = 17
UNROLL_A = 16
UNROLL_B = 16
OWN_FLOPS = 2_000_000_000
UNPACK_FLOPS = 1_000_000_000


SPACES = {"vmem": VMEM, "hbm": VMEM, "": VMEM, "smem": SMEM, "table": SMEM, "raw": pltpu.HBM}


def call(kernel, outs, ins, scratch=(), flops=0, aliases=None):
    args = [
        a
        if INTERPRET
        else pltpu.with_memory_space_constraint(a, VMEM if m == "vmem" else pltpu.HBM)
        if m in ("vmem", "hbm", "table", "raw")
        else a
        for a, m in ins
    ]
    shapes = [
        VMEM(shape, dtype) if m == "vmem" and not INTERPRET else jax.ShapeDtypeStruct(shape, dtype)
        for shape, dtype, m in outs
    ]
    return pl.pallas_call(
        kernel,
        out_shape=shapes,
        in_specs=[pl.BlockSpec(memory_space=SPACES[m]) for _, m in ins],
        out_specs=[pl.BlockSpec(memory_space=SPACES[m]) for _, _, m in outs],
        scratch_shapes=scratch,
        interpret=INTERPRET,
        input_output_aliases=aliases or {},
        compiler_params=pltpu.CompilerParams(vmem_limit_bytes=24 * 1024 * 1024),
        cost_estimate=pl.CostEstimate(flops=flops, bytes_accessed=0, transcendentals=0),
    )(*args)


def lanes(shape=(1, 128)):
    return lax.broadcasted_iota(jnp.int32, shape, len(shape) - 1)


def pack_kernel(dest, counts, elem, pos, vel, coef, send, block, own_elem):
    me = lax.axis_index("gy")
    lane = lanes()
    ids = lax.broadcasted_iota(jnp.int32, (8, 128), 0) * 128 + lanes((8, 128))

    def one(b, state):
        taken, labels = state
        d = dest[b] ^ me
        r = (taken >> (8 * d)) & 255
        block[d * SHARE + r] = b
        base = d * ROWS + r
        send[pl.ds(base, 3, stride=32), :] = pos[pl.ds(b, 3, stride=128), :]
        send[pl.ds(base + 96, 3, stride=32), :] = vel[pl.ds(b, 3, stride=128), :]
        rate = coef[pl.ds(2 * b, 1), :]
        send[pl.ds(base + 192, 1), :] = jnp.where(lane < counts[b], rate, 0.0)
        send[pl.ds(base + 224, 1), :] = coef[pl.ds(2 * b + 1, 1), :]
        own_elem[d * SHARE + r] = elem[b]
        labels = jnp.where(ids == d * 128 + r, elem[b], labels)
        return (taken + (1 << (8 * d)), labels)

    _, labels = lax.fori_loop(0, 128, one, (jnp.int32(0), jnp.zeros((8, 128), jnp.int32)), unroll=8)
    labels = labels.astype(F32)
    for d in range(N_GY):
        send[d * ROWS + 256 : d * ROWS + 264, :] = jnp.broadcast_to(labels[d : d + 1, :], (8, 128))


def split_two(x):
    high = x.astype(BF16)
    low = (x - high.astype(F32)).astype(BF16)
    return high, low


def lagrange(x, nodes, first):
    out = nodes[8 * (first + 7) : 8 * (first + 8), :]
    for t in range(7):
        out = out * (x - nodes[8 * (first + t) : 8 * (first + t + 1), :])
    return out


def gauss(x, nodes, row):
    d = nodes[8 * row : 8 * row + 8, :] - x
    return jnp.exp(d * d * (-SHARPNESS))


def outer(a, b):
    return jnp.concatenate([a[j : j + 1, :] * b for j in range(8)], axis=0)


def spread_field(vel, field):
    low_half = lanes() < 64

    def one(xy, _):
        for c in range(3):
            for h in range(4):
                t = vel[c * 8 + xy, :, 128 * h : 128 * h + 128].astype(F32)
                turned = pltpu.roll(t, 64, 1)
                at = (xy * 24 + c * 8 + h) * PITCH
                field[pl.ds(at, 16), :] = jnp.where(low_half, t, turned)
                field[pl.ds(at + 4 * PITCH, 16), :] = jnp.where(low_half, turned, t)
        return 0

    lax.fori_loop(0, 8, one, 0)


def interpolate(group, element, field, nodes, fluid):
    def one(r, _):
        e = element(r)
        basis_r = lagrange(group[pl.ds(r, 1), :], nodes, 8)
        basis_s = lagrange(group[pl.ds(r + 32, 1), :], nodes, 0)
        basis_t = lagrange(group[pl.ds(r + 64, 1), :], nodes, 0)
        high, low = split_two(outer(basis_s, basis_t))
        nodal = field[pl.ds((e >> 4) * (24 * PITCH) + (e & 15), 24, stride=PITCH), :].astype(BF16)
        part = jnp.dot(nodal, jnp.concatenate([high, low], axis=0), preferred_element_type=F32)
        for c in range(3):
            fluid[pl.ds(c * 32 + r, 1), :] = jnp.sum(
                part[8 * c : 8 * c + 8, :] * basis_r, axis=0, keepdims=True
            )
        return 0

    lax.fori_loop(0, SHARE, one, 0, unroll=UNROLL_A)


def find_drag(group, fluid, drag):
    w = [
        fluid[32 * c : 32 * c + 32, :] - group[96 + 32 * c : 128 + 32 * c, :] for c in range(3)
    ]
    scale = group[224:256, :]
    square = (w[0] * w[0] + w[1] * w[1] + w[2] * w[2]) * (scale * scale)
    power = jnp.where(square > 0.0, jnp.exp(0.3435 * jnp.log(square)), 0.0)
    factor = group[192:224, :] * (1.0 + 0.15 * power)
    for c in range(3):
        drag[32 * c : 32 * c + 32, :] = factor * w[c]


def project(group, element, drag, nodes, parts):
    low_half = lanes() < 64
    upper_rows = lax.broadcasted_iota(jnp.int32, (8, 128), 0) < 4

    def one(r, _):
        e = element(r)
        x = group[pl.ds(r, 1), :]
        near = [gauss(x, nodes, 17 + k) for k in range(2)]
        after = [gauss(x, nodes, 19 + k) for k in range(2)]
        planes = outer(
            gauss(group[pl.ds(r + 32, 1), :], nodes, 16),
            gauss(group[pl.ds(r + 64, 1), :], nodes, 16),
        )
        planes = jnp.concatenate(split_two(planes), axis=0)
        force = [-drag[pl.ds(c * 32 + r, 1), :] for c in range(3)]
        mixed = jnp.where(upper_rows, force[0], force[1])
        rows = []
        for k in range(2):
            rows += [near[k] * f for f in force] + [after[k] * mixed, after[k] * force[2]]
        rows = jnp.concatenate(split_two(jnp.concatenate(rows, axis=0)), axis=0)
        both = lax.dot_general(
            rows, planes, (((1,), (1,)), ((), ())), preferred_element_type=F32
        )
        both = both[:80, :] + both[80:, :]
        at = (e >> 4) * (36 * PITCH) + (e & 15)
        for k in range(5):
            even = both[8 * k : 8 * k + 8, :]
            odd = both[40 + 8 * k : 48 + 8 * k, :]
            t = jnp.where(low_half, even, odd)
            t = t + pltpu.roll(jnp.where(low_half, odd, even), 64, 1)
            n = 8 if k < 4 else 4
            parts[pl.ds(at + k * 8 * PITCH, n, stride=PITCH), :] = t[0:n, :]
        return 0

    lax.fori_loop(0, SHARE, one, 0, unroll=UNROLL_B)


def own_kernel(elem, group, vel, nodes, field, parts, drag, table, fluid):
    def element(r):
        return elem[r]

    table[...] = nodes[...]
    spread_field(vel, field)
    interpolate(group, element, field, nodes, fluid)
    find_drag(group, fluid, drag)
    project(group, element, drag, nodes, parts)


def rest_kernel(
    g1, g2, g3, field, nodes, _, d1, d2, d3, inside, ghosts, parts, fluid, lab_v, lab_s, sem
):
    groups = (g1, g2, g3)
    drags = (d1, d2, d3)
    for k, g in enumerate(groups):
        lab_v[k : k + 1, :] = g[256:257, :].astype(jnp.int32)
    copy = pltpu.make_async_copy(lab_v, lab_s, sem)
    copy.start()
    copy.wait()
    elements = [lambda r, k=k: lab_s[k, r] for k in range(3)]
    for k in range(3):
        interpolate(groups[k], elements[k], field, nodes, fluid)
        find_drag(groups[k], fluid, drags[k])
    for k in range(3):
        project(groups[k], elements[k], drags[k], nodes, parts)
    gather_parts(parts, inside, ghosts)


def gather_parts(parts, inside, ghosts):
    low_half = lanes() < 64
    odd = lax.axis_index("gx") & 1
    to_lo = (1 - odd) * 12
    to_hi = odd * 12

    def part(x, y, c, k, h):
        n = 2 * c + k if k < 2 else 6 + c
        return parts[pl.ds(((x * 4 + y) * 36 + n * 4 + h) * PITCH, 16), :]

    def one(y, _):
        for c in range(3):
            lower = []
            upper = []
            for h in range(4):
                lo = part(0, y, c, 1, h) + part(1, y, c, 0, h)
                hi = part(1, y, c, 1, h) + part(0, y, c, 2, h)
                inside[c * 8 + y, :, 128 * h : 128 * h + 128] = lo
                inside[c * 8 + 4 + y, :, 128 * h : 128 * h + 128] = hi
                lower.append(lo)
                upper.append(hi)
            for h in range(4):
                lo = part(0, y, c, 0, h)
                hi = part(1, y, c, 2, h)
                if h == 3:
                    lo = lo + jnp.where(low_half, 0.0, pltpu.roll(lower[0], 64, 1))
                if h == 0:
                    hi = hi + jnp.where(low_half, pltpu.roll(upper[3], 64, 1), 0.0)
                ghosts[to_lo + c * 4 + y, :, 128 * h : 128 * h + 128] = lo
                ghosts[to_hi + c * 4 + y, :, 128 * h : 128 * h + 128] = hi
        return 0

    lax.fori_loop(0, 4, one, 0)


def first_pass_kernel(last_gx, inside, sent, near, far, field, faces):
    low_half = lanes() < 64
    spot = (lanes() % 64) // 8
    gx = lax.axis_index("gx")
    odd = (gx & 1) == 1
    has_before = gx > 0
    has_after = gx < last_gx
    to_lo = (1 - (gx & 1)) * 12
    to_hi = (gx & 1) * 12
    y_odd = (lax.axis_index("gy") & 1) == 1

    def cut(ref, at, h):
        return ref[at, :, 128 * h : 128 * h + 128]

    for c in range(3):
        packed = [jnp.zeros((16, 128), F32), jnp.zeros((16, 128), F32)]
        for y in range(4):
            pair = [(cut(near, c * 4 + y, h), cut(far, c * 4 + y, h)) for h in range(4)]
            got_lo = [jnp.where(odd, n, f) for n, f in pair]
            got_hi = [jnp.where(odd, f, n) for n, f in pair]
            lower = [cut(inside, c * 8 + y, h) + got_lo[h] for h in range(4)]
            upper = [cut(inside, c * 8 + 4 + y, h) + got_hi[h] for h in range(4)]
            first = got_lo[0] + pltpu.roll(cut(sent, to_lo + c * 4 + y, 3), 64, 1)
            last = got_hi[3] + pltpu.roll(cut(sent, to_hi + c * 4 + y, 0), 64, 1)
            low3, up0 = lower[3], upper[0]
            lower[0] = jnp.where(low_half & has_before, first, lower[0])
            upper[3] = jnp.where(low_half | jnp.logical_not(has_after), upper[3], last)
            lower[3] = jnp.where(low_half, low3, low3 + pltpu.roll(up0, 64, 1))
            upper[0] = jnp.where(low_half, up0 + pltpu.roll(low3, 64, 1), up0)
            for x, layer in ((0, lower), (1, upper)):
                for h in range(4):
                    field[c * 8 + x * 4 + y, :, 128 * h : 128 * h + 128] = layer[h]
                    k = x * 4 + h
                    if y == 0:
                        moved = pltpu.roll(layer[h], 8 * k, 1) if k else layer[h]
                        packed[0] = jnp.where(spot == k, moved, packed[0])
                    if y == 3:
                        by = (8 * k - 56) % 128
                        moved = pltpu.roll(layer[h], by, 1) if by else layer[h]
                        packed[1] = jnp.where(spot == k, moved, packed[1])
        faces[16 * c : 16 * c + 16, :] = jnp.where(y_odd, packed[0], packed[1])
        faces[48 + 16 * c : 64 + 16 * c, :] = jnp.where(y_odd, packed[1], packed[0])


def last_passes(field, rows, before, after, buf, start):
    lane = lanes()
    bottom = (lane % 64) < 8
    top = (lane % 64) >= 56
    z = lax.broadcasted_iota(jnp.int32, (16, 128), 0)
    lane16 = lanes((16, 128))
    up_here = (lane16 % 8 == 7) & (z < 15)
    down_here = (lane16 % 8 == 0) & (z > 0)

    def one_comp(c, _):
        lo_pack = before(c)
        hi_pack = after(c)
        for x in range(2):
            for y in rows:
                for h in range(4):
                    k = x * 4 + h

                    def at(row):
                        return field[c * 8 + x * 4 + row, :, 128 * h : 128 * h + 128]

                    if y == 3:
                        above = hi_pack if k == 7 else pltpu.roll(hi_pack, 56 - 8 * k, 1)
                    else:
                        above = pltpu.roll(at(y + 1), 56, 1)
                    if y == 0:
                        below = lo_pack if k == 0 else pltpu.roll(lo_pack, 128 - 8 * k, 1)
                    else:
                        below = pltpu.roll(at(y - 1), 72, 1)
                    g = at(y) + jnp.where(top, above, jnp.where(bottom, below, 0.0))
                    above = pltpu.roll(pltpu.roll(g, 7, 1), 15, 0)
                    below = pltpu.roll(pltpu.roll(g, 121, 1), 1, 0)
                    g = g + jnp.where(up_here, above, jnp.where(down_here, below, 0.0))
                    buf[c * 8 + x * 4 + y, :, 128 * h : 128 * h + 128] = g
                start(c * 8 + x * 4 + y)
        return 0

    lax.fori_loop(0, 3, one_comp, 0)


def inner_kernel(block, field, d0, d1, d2, d3, drag, out, drag_buf, buf, sem, drag_sem):
    def copy(row):
        return pltpu.make_async_copy(buf.at[row], out.at[row], sem.at[row])

    last_passes(field, (1, 2), lambda c: None, lambda c: None, buf, lambda row: copy(row).start())
    for k, d in enumerate((d0, d1, d2, d3)):

        def one(r, _):
            drag_buf[pl.ds(block[k * SHARE + r], 3, stride=128), :] = d[pl.ds(r, 3, stride=32), :]
            return 0

        lax.fori_loop(0, SHARE, one, 0, unroll=8)
    moves = [
        pltpu.make_async_copy(
            drag_buf.at[pl.ds(96 * k, 96)], drag.at[pl.ds(96 * k, 96)], drag_sem.at[k]
        )
        for k in range(4)
    ]
    for move in moves:
        move.start()
    for row in range(24):
        if row % 4 in (1, 2):
            copy(row).wait()
    for move in moves:
        move.wait()


def outer_kernel(field, got1, got3, _, out, buf, sem):
    odd = (lax.axis_index("gy") & 1) == 1

    def copy(row):
        return pltpu.make_async_copy(buf.at[row], out.at[row], sem.at[row])

    def face(c, first):
        a = got1[pl.ds(16 * c, 16), :]
        b = got3[pl.ds(16 * c, 16), :]
        return jnp.where(odd, a, b) if first else jnp.where(odd, b, a)

    last_passes(
        field,
        (0, 3),
        lambda c: face(c, True),
        lambda c: face(c, False),
        buf,
        lambda row: copy(row).start(),
    )
    for row in range(24):
        if row % 4 in (0, 3):
            copy(row).wait()


def swapped(x, axis, partner):
    count = lax.axis_size(axis)
    pairs = [(i, partner(i)) for i in range(count) if 0 <= partner(i) < count]
    return lax.ppermute(x, axis, pairs)


def body(velocity, part_pos, part_vel, part_coef, counts, dest, elem):
    pos = part_pos.transpose(1, 0, 2).reshape(384, 128)
    vel = part_vel.transpose(1, 0, 2).reshape(384, 128)
    coef = part_coef.reshape(256, 128)
    nodes = jnp.asarray(node_table())
    send, block, own_elem = call(
        pack_kernel,
        [((N_GY * ROWS, 128), F32, "vmem"), ((128,), jnp.int32, "smem"), ((128,), jnp.int32, "smem")],
        [(dest, "table"), (counts, "table"), (elem, "table"), (pos, "hbm"), (vel, "hbm"), (coef, "hbm")],
    )
    own = send[:ROWS]
    groups = [
        swapped(send[k * ROWS : (k + 1) * ROWS], "gy", lambda i, k=k: i ^ k) for k in range(1, N_GY)
    ]
    field, parts, drag_own, table = call(
        own_kernel,
        [((8 * 24 * PITCH, 128), F32, "vmem"), ((8 * 36 * PITCH, 128), F32, "vmem"), ((96, 128), F32, "vmem"), (nodes.shape, F32, "vmem")],
        [(own_elem, "smem"), (own, "vmem"), (velocity.reshape(24, 16, 512), "hbm"), (nodes, "hbm")],
        (VMEM((96, 128), F32),),
        flops=OWN_FLOPS,
    )
    *drags, inside, ghosts, _ = call(
        rest_kernel,
        [((96, 128), F32, "vmem")] * 3
        + [((24, 16, 512), F32, "vmem")] * 2
        + [((8 * 36 * PITCH, 128), F32, "vmem")],
        [(g, "vmem") for g in groups] + [(field, "vmem"), (table, "vmem"), (parts, "vmem")],
        (
            VMEM((96, 128), F32),
            VMEM((8, 128), jnp.int32),
            SMEM((8, 128), jnp.int32),
            pltpu.SemaphoreType.DMA,
        ),
        aliases={5: 5},
    )
    far = swapped(ghosts[12:], "gx", lambda i: i + 1 if i & 1 else i - 1)
    near = swapped(ghosts[:12], "gx", lambda i: i ^ 1)
    back = [swapped(d, "gy", lambda i, k=k: i ^ k) for k, d in enumerate(drags, 1)]
    last_gx = lax.axis_size("gx") - 1
    field, faces = call(
        lambda *refs: first_pass_kernel(last_gx, *refs),
        [((24, 16, 512), F32, "vmem"), ((96, 128), F32, "vmem")],
        [(inside, "vmem"), (ghosts, "vmem"), (near, "vmem"), (far, "vmem")],
    )
    got1 = swapped(faces[:48], "gy", lambda i: i ^ 1)
    got3 = lax.ppermute(faces[48:], "gy", [(1, 2), (2, 1)])
    grid = (24, 16, 512)
    drag, out = call(
        inner_kernel,
        [((384, 128), F32, "raw"), (grid, F32, "raw")],
        [(block, "smem"), (field, "vmem"), (drag_own, "vmem")] + [(d, "vmem") for d in back],
        (
            VMEM((384, 128), F32),
            VMEM(grid, F32),
            pltpu.SemaphoreType.DMA((24,)),
            pltpu.SemaphoreType.DMA((4,)),
        ),
        flops=UNPACK_FLOPS,
    )
    (out,) = call(
        outer_kernel,
        [(grid, F32, "raw")],
        [(field, "vmem"), (got1, "vmem"), (got3, "vmem"), (out, "raw")],
        (VMEM(grid, F32), pltpu.SemaphoreType.DMA((24,))),
        aliases={3: 0},
    )
    return (
        drag.reshape(3, 128, 128).transpose(1, 0, 2),
        out.reshape(velocity.shape),
    )


def solution(mesh):
    in_specs = (
        P(None, "gx", "gy", None, None),
        P(("gx", "gy"), None, None),
        P(("gx", "gy"), None, None),
        P(("gx", "gy"), None, None),
        P(("gx", "gy")),
        P(("gx", "gy")),
        P(("gx", "gy")),
    )
    out_specs = (P(("gx", "gy"), None, None), P(None, "gx", "gy", None, None))
    return jax.shard_map(body, mesh=mesh, in_specs=in_specs, out_specs=out_specs, check_vma=False)
```

```python
import jax
import jax.numpy as jnp
import numpy as np
from jax import lax
from jax.experimental import pallas as pl
from jax.experimental.pallas import tpu as pltpu
from jax.sharding import PartitionSpec as P

GLL = (
    -1.0,
    -0.8717401485096066,
    -0.5917001814331423,
    -0.2092992179024789,
    0.2092992179024789,
    0.5917001814331423,
    0.8717401485096066,
    1.0,
)
SHARPNESS = 8.0
INTERPRET = False
F32 = jnp.float32
BF16 = jnp.bfloat16
VMEM = pltpu.VMEM
SMEM = pltpu.SMEM
N_GY = 4
SHARE = 32
ROWS = 264
PAIRED = (0, 2, 4, 6, 1, 3, 5, 7)


def node_table():
    q = np.array(GLL, np.float64)
    rows = []
    for order in (tuple(range(8)), PAIRED):
        for t in range(7):
            rows.append([q[[m for m in range(8) if m != i][t]] for i in order])
        rows.append([1.0 / np.prod([q[i] - q[m] for m in range(8) if m != i]) for i in order])
    rows.append([q[i] for i in range(8)])
    for first, second in ((-2.0, 0.0), (2.0, 2.0)):
        for half in (PAIRED[:4], PAIRED[4:]):
            rows.append([q[i] + first for i in half] + [q[i] + second for i in half])
    table = np.array(rows, np.float32).reshape(-1, 1)
    return np.ascontiguousarray(np.broadcast_to(table, (table.shape[0], 128)))


PITCH = 17
ORDER = (3, 1, 2)
UNROLL_A = 16
UNROLL_B = 16
OWN_FLOPS = 2_000_000_000
UNPACK_FLOPS = 1_000_000_000


SPACES = {"vmem": VMEM, "hbm": VMEM, "": VMEM, "smem": SMEM, "table": SMEM, "raw": pltpu.HBM}


def call(kernel, outs, ins, scratch=(), flops=0, aliases=None):
    args = [
        a
        if INTERPRET
        else pltpu.with_memory_space_constraint(a, VMEM if m == "vmem" else pltpu.HBM)
        if m in ("vmem", "hbm", "table", "raw")
        else a
        for a, m in ins
    ]
    shapes = [
        VMEM(shape, dtype) if m == "vmem" and not INTERPRET else jax.ShapeDtypeStruct(shape, dtype)
        for shape, dtype, m in outs
    ]
    return pl.pallas_call(
        kernel,
        out_shape=shapes,
        in_specs=[pl.BlockSpec(memory_space=SPACES[m]) for _, m in ins],
        out_specs=[pl.BlockSpec(memory_space=SPACES[m]) for _, _, m in outs],
        scratch_shapes=scratch,
        interpret=INTERPRET,
        input_output_aliases=aliases or {},
        compiler_params=pltpu.CompilerParams(vmem_limit_bytes=24 * 1024 * 1024),
        cost_estimate=pl.CostEstimate(flops=flops, bytes_accessed=0, transcendentals=0),
    )(*args)


def lanes(shape=(1, 128)):
    return lax.broadcasted_iota(jnp.int32, shape, len(shape) - 1)


def pack_kernel(
    dest_hbm, counts_hbm, elem_hbm, pos_hbm, vel_hbm, coef_hbm,
    send, block, own_elem,
    dest, counts, elem, pos, vel, coef, sem,
):
    tables = [
        pltpu.make_async_copy(a, b, sem.at[k])
        for k, (a, b) in enumerate(((dest_hbm, dest), (counts_hbm, counts), (elem_hbm, elem)))
    ]
    halves = []
    for k in range(2):
        cut = pl.ds(64 * k, 64)
        pairs = (
            (pos_hbm.at[:, cut], pos.at[:, cut]),
            (vel_hbm.at[:, cut], vel.at[:, cut]),
            (coef_hbm.at[pl.ds(128 * k, 128)], coef.at[pl.ds(128 * k, 128)]),
        )
        halves.append(
            [pltpu.make_async_copy(a, b, sem.at[3 + 3 * k + n]) for n, (a, b) in enumerate(pairs)]
        )
    for copy in tables + halves[0] + halves[1]:
        copy.start()
    me = lax.axis_index("gy")
    lane = lanes()
    ids = lax.broadcasted_iota(jnp.int32, (8, 128), 0) * 128 + lanes((8, 128))

    def one(b, state):
        taken, labels = state
        d = dest[b] ^ me
        r = (taken >> (8 * d)) & 255
        e = elem[b]
        block[d * SHARE + r] = b
        own_elem[d * SHARE + r] = e
        base = d * ROWS + r
        send[pl.ds(base, 3, stride=32), :] = pos[:, b, :]
        send[pl.ds(base + 96, 3, stride=32), :] = vel[:, b, :]
        rate = coef[pl.ds(2 * b, 1), :]
        send[pl.ds(base + 192, 1), :] = jnp.where(lane < counts[b], rate, 0.0)
        send[pl.ds(base + 224, 1), :] = coef[pl.ds(2 * b + 1, 1), :]
        labels = jnp.where(ids == d * 128 + r, e, labels)
        return (taken + (1 << (8 * d)), labels)

    state = (jnp.int32(0), jnp.zeros((8, 128), jnp.int32))
    for copy in tables:
        copy.wait()
    for k in range(2):
        for copy in halves[k]:
            copy.wait()
        state = lax.fori_loop(64 * k, 64 * k + 64, one, state, unroll=8)
    labels = state[1].astype(F32)
    for d in range(N_GY):
        send[d * ROWS + 256 : d * ROWS + 264, :] = jnp.broadcast_to(labels[d : d + 1, :], (8, 128))


def split_two(x):
    high = x.astype(BF16)
    low = (x - high.astype(F32)).astype(BF16)
    return high, low


def lagrange(x, nodes, first):
    out = nodes[8 * (first + 7) : 8 * (first + 8), :]
    for t in range(7):
        out = out * (x - nodes[8 * (first + t) : 8 * (first + t + 1), :])
    return out


def gauss(x, nodes, row):
    d = nodes[8 * row : 8 * row + 8, :] - x
    return jnp.exp(d * d * (-SHARPNESS))


def outer(a, b):
    return jnp.concatenate([a[j : j + 1, :] * b for j in range(8)], axis=0)


def spread_field(vel, field):
    low_half = lanes() < 64

    def one(xy, _):
        for c in range(3):
            for h in range(4):
                t = vel[c * 8 + xy, :, 128 * h : 128 * h + 128].astype(F32)
                turned = pltpu.roll(t, 64, 1)
                at = (xy * 24 + c * 8 + h) * PITCH
                field[pl.ds(at, 16), :] = jnp.where(low_half, t, turned)
                field[pl.ds(at + 4 * PITCH, 16), :] = jnp.where(low_half, turned, t)
        return 0

    lax.fori_loop(0, 8, one, 0)


def interpolate(group, element, field, nodes, fluid):
    def one(r, _):
        e = element(r)
        basis_r = lagrange(group[pl.ds(r, 1), :], nodes, 8)
        basis_s = lagrange(group[pl.ds(r + 32, 1), :], nodes, 0)
        basis_t = lagrange(group[pl.ds(r + 64, 1), :], nodes, 0)
        high, low = split_two(outer(basis_s, basis_t))
        nodal = field[pl.ds((e >> 4) * (24 * PITCH) + (e & 15), 24, stride=PITCH), :].astype(BF16)
        part = jnp.dot(nodal, jnp.concatenate([high, low], axis=0), preferred_element_type=F32)
        for c in range(3):
            fluid[pl.ds(c * 32 + r, 1), :] = jnp.sum(
                part[8 * c : 8 * c + 8, :] * basis_r, axis=0, keepdims=True
            )
        return 0

    lax.fori_loop(0, SHARE, one, 0, unroll=UNROLL_A)


def find_drag(group, fluid, drag):
    w = [
        fluid[32 * c : 32 * c + 32, :] - group[96 + 32 * c : 128 + 32 * c, :] for c in range(3)
    ]
    scale = group[224:256, :]
    square = (w[0] * w[0] + w[1] * w[1] + w[2] * w[2]) * (scale * scale)
    power = jnp.where(square > 0.0, jnp.exp(0.3435 * jnp.log(square)), 0.0)
    factor = group[192:224, :] * (1.0 + 0.15 * power)
    for c in range(3):
        drag[32 * c : 32 * c + 32, :] = factor * w[c]


def project(group, element, drag, nodes, parts):
    low_half = lanes() < 64
    upper_rows = lax.broadcasted_iota(jnp.int32, (8, 128), 0) < 4

    def one(r, _):
        e = element(r)
        x = group[pl.ds(r, 1), :]
        near = [gauss(x, nodes, 17 + k) for k in range(2)]
        after = [gauss(x, nodes, 19 + k) for k in range(2)]
        planes = outer(
            gauss(group[pl.ds(r + 32, 1), :], nodes, 16),
            gauss(group[pl.ds(r + 64, 1), :], nodes, 16),
        )
        planes = jnp.concatenate(split_two(planes), axis=0)
        force = [-drag[pl.ds(c * 32 + r, 1), :] for c in range(3)]
        mixed = jnp.where(upper_rows, force[0], force[1])
        rows = []
        for k in range(2):
            rows += [near[k] * f for f in force] + [after[k] * mixed, after[k] * force[2]]
        rows = jnp.concatenate(split_two(jnp.concatenate(rows, axis=0)), axis=0)
        both = lax.dot_general(
            rows, planes, (((1,), (1,)), ((), ())), preferred_element_type=F32
        )
        both = both[:80, :] + both[80:, :]
        at = (e >> 4) * (36 * PITCH) + (e & 15)
        for k in range(5):
            even = both[8 * k : 8 * k + 8, :]
            odd = both[40 + 8 * k : 48 + 8 * k, :]
            t = jnp.where(low_half, even, odd)
            t = t + pltpu.roll(jnp.where(low_half, odd, even), 64, 1)
            n = 8 if k < 4 else 4
            parts[pl.ds(at + k * 8 * PITCH, n, stride=PITCH), :] = t[0:n, :]
        return 0

    lax.fori_loop(0, SHARE, one, 0, unroll=UNROLL_B)


def own_kernel(elem, group, vel, nodes, field, parts, drag, table, fluid):
    def element(r):
        return elem[r]

    table[...] = nodes[...]
    spread_field(vel, field)
    interpolate(group, element, field, nodes, fluid)
    find_drag(group, fluid, drag)
    project(group, element, drag, nodes, parts)


def rest_kernel(
    g1, g2, g3, field, nodes, _, d1, d2, d3, inside, ghosts, parts, fluid, lab_v, lab_s, sem
):
    groups = (g1, g2, g3)
    drags = (d1, d2, d3)
    for k, g in enumerate(groups):
        lab_v[k : k + 1, :] = g[256:257, :].astype(jnp.int32)
    copy = pltpu.make_async_copy(lab_v, lab_s, sem)
    copy.start()
    copy.wait()
    elements = [lambda r, k=k: lab_s[k, r] for k in range(3)]
    for k in range(3):
        interpolate(groups[k], elements[k], field, nodes, fluid)
        find_drag(groups[k], fluid, drags[k])
    for k in range(3):
        project(groups[k], elements[k], drags[k], nodes, parts)
    gather_parts(parts, inside, ghosts)


def gather_parts(parts, inside, ghosts):
    low_half = lanes() < 64
    odd = lax.axis_index("gx") & 1
    to_lo = (1 - odd) * 12
    to_hi = odd * 12

    def part(x, y, c, k, h):
        n = 2 * c + k if k < 2 else 6 + c
        return parts[pl.ds(((x * 4 + y) * 36 + n * 4 + h) * PITCH, 16), :]

    def one(y, _):
        for c in range(3):
            lower = []
            upper = []
            for h in range(4):
                lo = part(0, y, c, 1, h) + part(1, y, c, 0, h)
                hi = part(1, y, c, 1, h) + part(0, y, c, 2, h)
                inside[c * 8 + y, :, 128 * h : 128 * h + 128] = lo
                inside[c * 8 + 4 + y, :, 128 * h : 128 * h + 128] = hi
                lower.append(lo)
                upper.append(hi)
            for h in range(4):
                lo = part(0, y, c, 0, h)
                hi = part(1, y, c, 2, h)
                if h == 3:
                    lo = lo + jnp.where(low_half, 0.0, pltpu.roll(lower[0], 64, 1))
                if h == 0:
                    hi = hi + jnp.where(low_half, pltpu.roll(upper[3], 64, 1), 0.0)
                ghosts[to_lo + c * 4 + y, :, 128 * h : 128 * h + 128] = lo
                ghosts[to_hi + c * 4 + y, :, 128 * h : 128 * h + 128] = hi
        return 0

    lax.fori_loop(0, 4, one, 0)


def first_pass_kernel(last_gx, inside, sent, near, far, field, faces):
    low_half = lanes() < 64
    spot = (lanes() % 64) // 8
    gx = lax.axis_index("gx")
    odd = (gx & 1) == 1
    has_before = gx > 0
    has_after = gx < last_gx
    to_lo = (1 - (gx & 1)) * 12
    to_hi = (gx & 1) * 12
    y_odd = (lax.axis_index("gy") & 1) == 1

    def cut(ref, at, h):
        return ref[at, :, 128 * h : 128 * h + 128]

    for c in range(3):
        packed = [jnp.zeros((16, 128), F32), jnp.zeros((16, 128), F32)]
        for y in range(4):
            pair = [(cut(near, c * 4 + y, h), cut(far, c * 4 + y, h)) for h in range(4)]
            got_lo = [jnp.where(odd, n, f) for n, f in pair]
            got_hi = [jnp.where(odd, f, n) for n, f in pair]
            lower = [
                cut(inside, c * 8 + y, h) + jnp.where(has_before, got_lo[h], 0.0) for h in range(4)
            ]
            upper = [
                cut(inside, c * 8 + 4 + y, h) + jnp.where(has_after, got_hi[h], 0.0)
                for h in range(4)
            ]
            first = got_lo[0] + pltpu.roll(cut(sent, to_lo + c * 4 + y, 3), 64, 1)
            last = got_hi[3] + pltpu.roll(cut(sent, to_hi + c * 4 + y, 0), 64, 1)
            low3, up0 = lower[3], upper[0]
            lower[0] = jnp.where(low_half & has_before, first, lower[0])
            upper[3] = jnp.where(low_half | jnp.logical_not(has_after), upper[3], last)
            lower[3] = jnp.where(low_half, low3, low3 + pltpu.roll(up0, 64, 1))
            upper[0] = jnp.where(low_half, up0 + pltpu.roll(low3, 64, 1), up0)
            for x, layer in ((0, lower), (1, upper)):
                for h in range(4):
                    field[c * 8 + x * 4 + y, :, 128 * h : 128 * h + 128] = layer[h]
                    k = x * 4 + h
                    if y == 0:
                        moved = pltpu.roll(layer[h], 8 * k, 1) if k else layer[h]
                        packed[0] = jnp.where(spot == k, moved, packed[0])
                    if y == 3:
                        by = (8 * k - 56) % 128
                        moved = pltpu.roll(layer[h], by, 1) if by else layer[h]
                        packed[1] = jnp.where(spot == k, moved, packed[1])
        faces[16 * c : 16 * c + 16, :] = jnp.where(y_odd, packed[0], packed[1])
        faces[48 + 16 * c : 64 + 16 * c, :] = jnp.where(y_odd, packed[1], packed[0])


def last_passes(field, rows, before, after, buf, start):
    lane = lanes()
    bottom = (lane % 64) < 8
    top = (lane % 64) >= 56
    z = lax.broadcasted_iota(jnp.int32, (16, 128), 0)
    lane16 = lanes((16, 128))
    up_here = (lane16 % 8 == 7) & (z < 15)
    down_here = (lane16 % 8 == 0) & (z > 0)

    def one_comp(c, _):
        lo_pack = before(c)
        hi_pack = after(c)
        for x in range(2):
            for y in rows:
                for h in range(4):
                    k = x * 4 + h

                    def at(row):
                        return field[c * 8 + x * 4 + row, :, 128 * h : 128 * h + 128]

                    if y == 3:
                        above = hi_pack if k == 7 else pltpu.roll(hi_pack, 56 - 8 * k, 1)
                    else:
                        above = pltpu.roll(at(y + 1), 56, 1)
                    if y == 0:
                        below = lo_pack if k == 0 else pltpu.roll(lo_pack, 128 - 8 * k, 1)
                    else:
                        below = pltpu.roll(at(y - 1), 72, 1)
                    g = at(y) + jnp.where(top, above, jnp.where(bottom, below, 0.0))
                    above = pltpu.roll(pltpu.roll(g, 7, 1), 15, 0)
                    below = pltpu.roll(pltpu.roll(g, 121, 1), 1, 0)
                    g = g + jnp.where(up_here, above, jnp.where(down_here, below, 0.0))
                    buf[c * 8 + x * 4 + y, :, 128 * h : 128 * h + 128] = g
                start(c * 8 + x * 4 + y)
        return 0

    lax.fori_loop(0, 3, one_comp, 0)


def inner_kernel(block, field, d0, d1, d2, d3, drag, out, drag_buf, buf, sem, drag_sem):
    def copy(row):
        return pltpu.make_async_copy(buf.at[row], out.at[row], sem.at[row])

    last_passes(field, (1, 2), lambda c: None, lambda c: None, buf, lambda row: copy(row).start())
    for k, d in enumerate((d0, d1, d2, d3)):

        def one(r, _):
            drag_buf[pl.ds(block[k * SHARE + r], 3, stride=128), :] = d[pl.ds(r, 3, stride=32), :]
            return 0

        lax.fori_loop(0, SHARE, one, 0, unroll=8)
    moves = [
        pltpu.make_async_copy(
            drag_buf.at[pl.ds(96 * k, 96)], drag.at[pl.ds(96 * k, 96)], drag_sem.at[k]
        )
        for k in range(4)
    ]
    for move in moves:
        move.start()
    for row in range(24):
        if row % 4 in (1, 2):
            copy(row).wait()
    for move in moves:
        move.wait()


def outer_kernel(field, got1, got3, _, out, buf, sem):
    gy = lax.axis_index("gy")
    odd = (gy & 1) == 1
    between = (gy > 0) & (gy < N_GY - 1)

    def copy(row):
        return pltpu.make_async_copy(buf.at[row], out.at[row], sem.at[row])

    def face(c, first):
        a = got1[pl.ds(16 * c, 16), :]
        b = jnp.where(between, got3[pl.ds(16 * c, 16), :], 0.0)
        return jnp.where(odd, a, b) if first else jnp.where(odd, b, a)

    last_passes(
        field,
        (0, 3),
        lambda c: face(c, True),
        lambda c: face(c, False),
        buf,
        lambda row: copy(row).start(),
    )
    for row in range(24):
        if row % 4 in (0, 3):
            copy(row).wait()


def swapped(x, axis, partner):
    count = lax.axis_size(axis)
    return lax.ppermute(x, axis, [(i, partner(i) % count) for i in range(count)])


def body(velocity, part_pos, part_vel, part_coef, counts, dest, elem):
    pos = part_pos.transpose(1, 0, 2)
    vel = part_vel.transpose(1, 0, 2)
    coef = part_coef.reshape(256, 128)
    nodes = jnp.asarray(node_table())
    send, block, own_elem = call(
        pack_kernel,
        [((N_GY * ROWS, 128), F32, "vmem"), ((128,), jnp.int32, "smem"), ((128,), jnp.int32, "smem")],
        [(a, "raw") for a in (dest, counts, elem, pos, vel, coef)],
        (SMEM((128,), jnp.int32),) * 3
        + (VMEM(pos.shape, F32),) * 2
        + (VMEM(coef.shape, F32), pltpu.SemaphoreType.DMA((9,))),
    )
    own = send[:ROWS]
    groups = {
        k: swapped(send[k * ROWS : (k + 1) * ROWS], "gy", lambda i, k=k: i ^ k) for k in ORDER
    }
    field, parts, drag_own, table = call(
        own_kernel,
        [((8 * 24 * PITCH, 128), F32, "vmem"), ((8 * 36 * PITCH, 128), F32, "vmem"), ((96, 128), F32, "vmem"), (nodes.shape, F32, "vmem")],
        [(own_elem, "smem"), (own, "vmem"), (velocity.reshape(24, 16, 512), "hbm"), (nodes, "hbm")],
        (VMEM((96, 128), F32),),
        flops=OWN_FLOPS,
    )
    *drags, inside, ghosts, _ = call(
        rest_kernel,
        [((96, 128), F32, "vmem")] * 3
        + [((24, 16, 512), F32, "vmem")] * 2
        + [((8 * 36 * PITCH, 128), F32, "vmem")],
        [(groups[k], "vmem") for k in ORDER] + [(field, "vmem"), (table, "vmem"), (parts, "vmem")],
        (
            VMEM((96, 128), F32),
            VMEM((8, 128), jnp.int32),
            SMEM((8, 128), jnp.int32),
            pltpu.SemaphoreType.DMA,
        ),
        aliases={5: 5},
    )
    far = swapped(ghosts[12:], "gx", lambda i: i + 1 if i & 1 else i - 1)
    near = swapped(ghosts[:12], "gx", lambda i: i ^ 1)
    back = {k: swapped(d, "gy", lambda i, k=k: i ^ k) for k, d in zip(ORDER, drags)}
    last_gx = lax.axis_size("gx") - 1
    field, faces = call(
        lambda *refs: first_pass_kernel(last_gx, *refs),
        [((24, 16, 512), F32, "vmem"), ((96, 128), F32, "vmem")],
        [(inside, "vmem"), (ghosts, "vmem"), (near, "vmem"), (far, "vmem")],
    )
    got1 = swapped(faces[:48], "gy", lambda i: i ^ 1)
    got3 = swapped(faces[48:], "gy", lambda i: i ^ 3)
    grid = (24, 16, 512)
    drag, out = call(
        inner_kernel,
        [((384, 128), F32, "raw"), (grid, F32, "raw")],
        [(block, "smem"), (field, "vmem"), (drag_own, "vmem")] + [(back[k], "vmem") for k in range(1, N_GY)],
        (
            VMEM((384, 128), F32),
            VMEM(grid, F32),
            pltpu.SemaphoreType.DMA((24,)),
            pltpu.SemaphoreType.DMA((4,)),
        ),
        flops=UNPACK_FLOPS,
    )
    (out,) = call(
        outer_kernel,
        [(grid, F32, "raw")],
        [(field, "vmem"), (got1, "vmem"), (got3, "vmem"), (out, "raw")],
        (VMEM(grid, F32), pltpu.SemaphoreType.DMA((24,))),
        aliases={3: 0},
    )
    return (
        drag.reshape(3, 128, 128).transpose(1, 0, 2),
        out.reshape(velocity.shape),
    )


def solution(mesh):
    in_specs = (
        P(None, "gx", "gy", None, None),
        P(("gx", "gy"), None, None),
        P(("gx", "gy"), None, None),
        P(("gx", "gy"), None, None),
        P(("gx", "gy")),
        P(("gx", "gy")),
        P(("gx", "gy")),
    )
    out_specs = (P(("gx", "gy"), None, None), P(None, "gx", "gy", None, None))
    return jax.shard_map(body, mesh=mesh, in_specs=in_specs, out_specs=out_specs, check_vma=False)
```

```python
import jax
import jax.numpy as jnp
import numpy as np
from jax import lax
from jax.experimental import pallas as pl
from jax.experimental.pallas import tpu as pltpu
from jax.sharding import PartitionSpec as P

GLL = (
    -1.0,
    -0.8717401485096066,
    -0.5917001814331423,
    -0.2092992179024789,
    0.2092992179024789,
    0.5917001814331423,
    0.8717401485096066,
    1.0,
)
SHARPNESS = 8.0
INTERPRET = False
F32 = jnp.float32
BF16 = jnp.bfloat16
VMEM = pltpu.VMEM
SMEM = pltpu.SMEM
N_GY = 4
SHARE = 32
ROWS = 264
PAIRED = (0, 2, 4, 6, 1, 3, 5, 7)


def node_table():
    q = np.array(GLL, np.float64)
    rows = []
    for order in (tuple(range(8)), PAIRED):
        for t in range(7):
            rows.append([q[[m for m in range(8) if m != i][t]] for i in order])
        rows.append([1.0 / np.prod([q[i] - q[m] for m in range(8) if m != i]) for i in order])
    rows.append([q[i] for i in range(8)])
    for first, second in ((-2.0, 0.0), (2.0, 2.0)):
        for half in (PAIRED[:4], PAIRED[4:]):
            rows.append([q[i] + first for i in half] + [q[i] + second for i in half])
    table = np.array(rows, np.float32).reshape(-1, 1)
    return np.ascontiguousarray(np.broadcast_to(table, (table.shape[0], 128)))


PITCH = 17
ORDER = (3, 1, 2)
UNROLL_A = 16
UNROLL_B = 16
OWN_FLOPS = 2_000_000_000
INNER_FLOPS = 1_000_000_000


SPACES = {"vmem": VMEM, "hbm": VMEM, "": VMEM, "smem": SMEM, "table": SMEM, "raw": pltpu.HBM}


def call(kernel, outs, ins, scratch=(), flops=0, aliases=None):
    args = [
        a
        if INTERPRET
        else pltpu.with_memory_space_constraint(a, VMEM if m == "vmem" else pltpu.HBM)
        if m in ("vmem", "hbm", "table", "raw")
        else a
        for a, m in ins
    ]
    shapes = [
        VMEM(shape, dtype) if m == "vmem" and not INTERPRET else jax.ShapeDtypeStruct(shape, dtype)
        for shape, dtype, m in outs
    ]
    return pl.pallas_call(
        kernel,
        out_shape=shapes,
        in_specs=[pl.BlockSpec(memory_space=SPACES[m]) for _, m in ins],
        out_specs=[pl.BlockSpec(memory_space=SPACES[m]) for _, _, m in outs],
        scratch_shapes=scratch,
        interpret=INTERPRET,
        input_output_aliases=aliases or {},
        compiler_params=pltpu.CompilerParams(vmem_limit_bytes=24 * 1024 * 1024),
        cost_estimate=pl.CostEstimate(flops=flops, bytes_accessed=0, transcendentals=0),
    )(*args)


def lanes(shape=(1, 128)):
    return lax.broadcasted_iota(jnp.int32, shape, len(shape) - 1)


def pack_kernel(
    dest_hbm, counts_hbm, elem_hbm, pos_hbm, vel_hbm, coef_hbm,
    send, block, own_elem,
    dest, counts, elem, pos, vel, coef, sem,
):
    tables = [
        pltpu.make_async_copy(a, b, sem.at[k])
        for k, (a, b) in enumerate(((dest_hbm, dest), (counts_hbm, counts), (elem_hbm, elem)))
    ]
    halves = []
    for k in range(2):
        cut = pl.ds(64 * k, 64)
        pairs = (
            (pos_hbm.at[:, cut], pos.at[:, cut]),
            (vel_hbm.at[:, cut], vel.at[:, cut]),
            (coef_hbm.at[pl.ds(128 * k, 128)], coef.at[pl.ds(128 * k, 128)]),
        )
        halves.append(
            [pltpu.make_async_copy(a, b, sem.at[3 + 3 * k + n]) for n, (a, b) in enumerate(pairs)]
        )
    for copy in tables + halves[0] + halves[1]:
        copy.start()
    me = lax.axis_index("gy")
    lane = lanes()
    ids = lax.broadcasted_iota(jnp.int32, (8, 128), 0) * 128 + lanes((8, 128))

    def one(b, state):
        taken, labels = state
        d = dest[b] ^ me
        r = (taken >> (8 * d)) & 255
        e = elem[b]
        block[d * SHARE + r] = b
        own_elem[d * SHARE + r] = e
        base = d * ROWS + r
        send[pl.ds(base, 3, stride=32), :] = pos[:, b, :]
        send[pl.ds(base + 96, 3, stride=32), :] = vel[:, b, :]
        rate = coef[pl.ds(2 * b, 1), :]
        send[pl.ds(base + 192, 1), :] = jnp.where(lane < counts[b], rate, 0.0)
        send[pl.ds(base + 224, 1), :] = coef[pl.ds(2 * b + 1, 1), :]
        labels = jnp.where(ids == d * 128 + r, e, labels)
        return (taken + (1 << (8 * d)), labels)

    state = (jnp.int32(0), jnp.zeros((8, 128), jnp.int32))
    for copy in tables:
        copy.wait()
    for k in range(2):
        for copy in halves[k]:
            copy.wait()
        state = lax.fori_loop(64 * k, 64 * k + 64, one, state, unroll=8)
    labels = state[1].astype(F32)
    for d in range(N_GY):
        send[d * ROWS + 256 : d * ROWS + 264, :] = jnp.broadcast_to(labels[d : d + 1, :], (8, 128))


def split_two(x):
    high = x.astype(BF16)
    low = (x - high.astype(F32)).astype(BF16)
    return high, low


def lagrange(x, nodes, first):
    out = nodes[8 * (first + 7) : 8 * (first + 8), :]
    for t in range(7):
        out = out * (x - nodes[8 * (first + t) : 8 * (first + t + 1), :])
    return out


def gauss(x, nodes, row):
    d = nodes[8 * row : 8 * row + 8, :] - x
    return jnp.exp(d * d * (-SHARPNESS))


def outer(a, b):
    return jnp.concatenate([a[j : j + 1, :] * b for j in range(8)], axis=0)


def spread_field(vel, field):
    low_half = lanes() < 64

    def one(xy, _):
        for c in range(3):
            for h in range(4):
                t = vel[c * 8 + xy, :, 128 * h : 128 * h + 128].astype(F32)
                turned = pltpu.roll(t, 64, 1)
                at = (xy * 24 + c * 8 + h) * PITCH
                field[pl.ds(at, 16), :] = jnp.where(low_half, t, turned)
                field[pl.ds(at + 4 * PITCH, 16), :] = jnp.where(low_half, turned, t)
        return 0

    lax.fori_loop(0, 8, one, 0)


def interpolate(group, element, field, nodes, fluid):
    def one(r, _):
        e = element(r)
        basis_r = lagrange(group[pl.ds(r, 1), :], nodes, 8)
        basis_s = lagrange(group[pl.ds(r + 32, 1), :], nodes, 0)
        basis_t = lagrange(group[pl.ds(r + 64, 1), :], nodes, 0)
        high, low = split_two(outer(basis_s, basis_t))
        nodal = field[pl.ds((e >> 4) * (24 * PITCH) + (e & 15), 24, stride=PITCH), :].astype(BF16)
        part = jnp.dot(nodal, jnp.concatenate([high, low], axis=0), preferred_element_type=F32)
        for c in range(3):
            fluid[pl.ds(c * 32 + r, 1), :] = jnp.sum(
                part[8 * c : 8 * c + 8, :] * basis_r, axis=0, keepdims=True
            )
        return 0

    lax.fori_loop(0, SHARE, one, 0, unroll=UNROLL_A)


def find_drag(group, fluid, drag):
    w = [
        fluid[32 * c : 32 * c + 32, :] - group[96 + 32 * c : 128 + 32 * c, :] for c in range(3)
    ]
    scale = group[224:256, :]
    square = (w[0] * w[0] + w[1] * w[1] + w[2] * w[2]) * (scale * scale)
    power = jnp.where(square > 0.0, jnp.exp(0.3435 * jnp.log(square)), 0.0)
    factor = group[192:224, :] * (1.0 + 0.15 * power)
    for c in range(3):
        drag[32 * c : 32 * c + 32, :] = factor * w[c]


def project(group, element, drag, nodes, parts):
    low_half = lanes() < 64
    upper_rows = lax.broadcasted_iota(jnp.int32, (8, 128), 0) < 4

    def one(r, _):
        e = element(r)
        x = group[pl.ds(r, 1), :]
        near = [gauss(x, nodes, 17 + k) for k in range(2)]
        after = [gauss(x, nodes, 19 + k) for k in range(2)]
        planes = outer(
            gauss(group[pl.ds(r + 32, 1), :], nodes, 16),
            gauss(group[pl.ds(r + 64, 1), :], nodes, 16),
        )
        planes = jnp.concatenate(split_two(planes), axis=0)
        force = [-drag[pl.ds(c * 32 + r, 1), :] for c in range(3)]
        mixed = jnp.where(upper_rows, force[0], force[1])
        rows = []
        for k in range(2):
            rows += [near[k] * f for f in force] + [after[k] * mixed, after[k] * force[2]]
        rows = jnp.concatenate(split_two(jnp.concatenate(rows, axis=0)), axis=0)
        both = lax.dot_general(
            rows, planes, (((1,), (1,)), ((), ())), preferred_element_type=F32
        )
        both = both[:80, :] + both[80:, :]
        at = (e >> 4) * (36 * PITCH) + (e & 15)
        for k in range(5):
            even = both[8 * k : 8 * k + 8, :]
            odd = both[40 + 8 * k : 48 + 8 * k, :]
            t = jnp.where(low_half, even, odd)
            t = t + pltpu.roll(jnp.where(low_half, odd, even), 64, 1)
            n = 8 if k < 4 else 4
            parts[pl.ds(at + k * 8 * PITCH, n, stride=PITCH), :] = t[0:n, :]
        return 0

    lax.fori_loop(0, SHARE, one, 0, unroll=UNROLL_B)


def own_kernel(elem, group, vel, nodes, field, parts, drag, table, fluid):
    def element(r):
        return elem[r]

    table[...] = nodes[...]
    spread_field(vel, field)
    interpolate(group, element, field, nodes, fluid)
    find_drag(group, fluid, drag)
    project(group, element, drag, nodes, parts)


def rest_kernel(
    g3, g1, g2, field, nodes, _, send3, send1, drag2, inside, ghosts, parts, fluid, lab_v, lab_s, sem
):
    groups = (g3, g1, g2)
    drags = (send3, send1, drag2)
    for k, g in enumerate(groups):
        lab_v[k : k + 1, :] = g[256:257, :].astype(jnp.int32)
    copy = pltpu.make_async_copy(lab_v, lab_s, sem)
    copy.start()
    copy.wait()
    elements = [lambda r, k=k: lab_s[k, r] for k in range(3)]
    for k in range(3):
        interpolate(groups[k], elements[k], field, nodes, fluid)
        find_drag(groups[k], fluid, drags[k])
    for k in range(3):
        project(groups[k], elements[k], drags[k], nodes, parts)
    gather_parts(parts, inside, ghosts, send1, send3)


def slots():
    return (lanes() % 64) // 8


def pack_face(layers, upper):
    spot = slots()
    out = jnp.zeros((16, 128), F32)
    for k, layer in enumerate(layers):
        by = (8 * k - 56 * upper) % 128
        out = jnp.where(spot == k, pltpu.roll(layer, by, 1) if by else layer, out)
    return out


def gather_parts(parts, inside, ghosts, send1, send3):
    low_half = lanes() < 64
    odd = lax.axis_index("gx") & 1
    to_lo = (1 - odd) * 12
    to_hi = odd * 12
    y_odd = (lax.axis_index("gy") & 1) == 1

    def part(x, y, c, k, h):
        n = 2 * c + k if k < 2 else 6 + c
        return parts[pl.ds(((x * 4 + y) * 36 + n * 4 + h) * PITCH, 16), :]

    for c in range(3):
        faces = {}
        for y in range(4):
            lower = [part(0, y, c, 1, h) + part(1, y, c, 0, h) for h in range(4)]
            upper = [part(1, y, c, 1, h) + part(0, y, c, 2, h) for h in range(4)]
            lo = [part(0, y, c, 0, h) for h in range(4)]
            hi = [part(1, y, c, 2, h) for h in range(4)]
            lo[3] = lo[3] + jnp.where(low_half, 0.0, pltpu.roll(lower[0], 64, 1))
            hi[0] = hi[0] + jnp.where(low_half, pltpu.roll(upper[3], 64, 1), 0.0)
            for h in range(4):
                cut = slice(128 * h, 128 * h + 128)
                inside[c * 8 + y, :, cut] = lower[h]
                inside[c * 8 + 4 + y, :, cut] = upper[h]
                ghosts[to_lo + c * 4 + y, :, cut] = lo[h]
                ghosts[to_hi + c * 4 + y, :, cut] = hi[h]
            if y in (0, 3):
                faces[y] = (pack_face(lower + upper, y == 3), pack_face(lo + hi, y == 3))
        for k in range(2):
            at = slice(96 + 48 * k + 16 * c, 112 + 48 * k + 16 * c)
            send1[at, :] = jnp.where(y_odd, faces[0][k], faces[3][k])
            send3[at, :] = jnp.where(y_odd, faces[3][k], faces[0][k])


def forward_kernel(got1, got3, near, far):
    low_slots = slots() < 4
    x_odd = (lax.axis_index("gx") & 1) == 1
    y_odd = (lax.axis_index("gy") & 1) == 1
    one = got1[144:192, :]
    three = got3[144:192, :]
    before = jnp.where(y_odd, one, three)
    after = jnp.where(y_odd, three, one)
    of_lo = jnp.where(low_slots, before, pltpu.roll(after, 32, 1))
    of_hi = jnp.where(low_slots, pltpu.roll(before, 96, 1), after)
    near[...] = jnp.where(x_odd, of_lo, of_hi)
    far[...] = jnp.where(x_odd, of_hi, of_lo)


def first_pass(last_gx, inside, sent, near, far, field):
    low_half = lanes() < 64
    gx = lax.axis_index("gx")
    odd = (gx & 1) == 1
    has_before = gx > 0
    has_after = gx < last_gx
    to_lo = (1 - (gx & 1)) * 12
    to_hi = (gx & 1) * 12

    def one_comp(c, _):
        for y in range(4):

            def cut(ref, at, h):
                return ref[at + c * 4 + y, :, 128 * h : 128 * h + 128]

            pair = [(cut(near, 0, h), cut(far, 0, h)) for h in range(4)]
            got_lo = [jnp.where(odd, n, f) for n, f in pair]
            got_hi = [jnp.where(odd, f, n) for n, f in pair]
            lower = [
                cut(inside, c * 4, h) + jnp.where(has_before, got_lo[h], 0.0) for h in range(4)
            ]
            upper = [
                cut(inside, c * 4 + 4, h) + jnp.where(has_after, got_hi[h], 0.0) for h in range(4)
            ]
            first = got_lo[0] + pltpu.roll(cut(sent, to_lo, 3), 64, 1)
            last = got_hi[3] + pltpu.roll(cut(sent, to_hi, 0), 64, 1)
            low3, up0 = lower[3], upper[0]
            lower[0] = jnp.where(low_half & has_before, first, lower[0])
            upper[3] = jnp.where(low_half | jnp.logical_not(has_after), upper[3], last)
            lower[3] = jnp.where(low_half, low3, low3 + pltpu.roll(up0, 64, 1))
            upper[0] = jnp.where(low_half, up0 + pltpu.roll(low3, 64, 1), up0)
            for h in range(4):
                field[c * 8 + y, :, 128 * h : 128 * h + 128] = lower[h]
                field[c * 8 + 4 + y, :, 128 * h : 128 * h + 128] = upper[h]
        return 0

    lax.fori_loop(0, 3, one_comp, 0)


def last_passes(field, rows, before, after, buf, start):
    lane = lanes()
    bottom = (lane % 64) < 8
    top = (lane % 64) >= 56
    z = lax.broadcasted_iota(jnp.int32, (16, 128), 0)
    lane16 = lanes((16, 128))
    up_here = (lane16 % 8 == 7) & (z < 15)
    down_here = (lane16 % 8 == 0) & (z > 0)

    def one_comp(c, _):
        lo_pack = before(c)
        hi_pack = after(c)
        for x in range(2):
            for y in rows:
                for h in range(4):
                    k = x * 4 + h

                    def at(row):
                        return field[c * 8 + x * 4 + row, :, 128 * h : 128 * h + 128]

                    if y == 3:
                        above = hi_pack if k == 7 else pltpu.roll(hi_pack, 56 - 8 * k, 1)
                    else:
                        above = pltpu.roll(at(y + 1), 56, 1)
                    if y == 0:
                        below = lo_pack if k == 0 else pltpu.roll(lo_pack, 128 - 8 * k, 1)
                    else:
                        below = pltpu.roll(at(y - 1), 72, 1)
                    g = at(y) + jnp.where(top, above, jnp.where(bottom, below, 0.0))
                    above = pltpu.roll(pltpu.roll(g, 7, 1), 15, 0)
                    below = pltpu.roll(pltpu.roll(g, 121, 1), 1, 0)
                    g = g + jnp.where(up_here, above, jnp.where(down_here, below, 0.0))
                    buf[c * 8 + x * 4 + y, :, 128 * h : 128 * h + 128] = g
                start(c * 8 + x * 4 + y)
        return 0

    lax.fori_loop(0, 3, one_comp, 0)


def inner_kernel(
    last_gx, block, inside, sent, near, far, d0, d1, d2, d3,
    drag, out, field, drag_buf, buf, sem, drag_sem,
):
    def copy(row):
        return pltpu.make_async_copy(buf.at[row], out.at[row], sem.at[row])

    for k, d in enumerate((d0, d1, d2, d3)):

        def one(r, _):
            drag_buf[pl.ds(block[k * SHARE + r], 3, stride=128), :] = d[pl.ds(r, 3, stride=32), :]
            return 0

        lax.fori_loop(0, SHARE, one, 0, unroll=8)
    first_pass(last_gx, inside, sent, near, far, field)
    moves = [
        pltpu.make_async_copy(
            drag_buf.at[pl.ds(96 * k, 96)], drag.at[pl.ds(96 * k, 96)], drag_sem.at[k]
        )
        for k in range(4)
    ]
    for move in moves:
        move.start()
    last_passes(field, (1, 2), lambda c: None, lambda c: None, buf, lambda row: copy(row).start())
    for row in range(24):
        if row % 4 in (1, 2):
            copy(row).wait()
    for move in moves:
        move.wait()


def outer_kernel(last_gx, field, got1, got3, near, far, _, out, buf, sem):
    gx = lax.axis_index("gx")
    x_odd = (gx & 1) == 1
    gy = lax.axis_index("gy")
    y_odd = (gy & 1) == 1
    has_before = gx > 0
    has_after = gx < last_gx
    lane = lanes()
    low_slots = slots() < 4
    here = (low_slots & has_before) | (jnp.logical_not(low_slots) & has_after)

    def copy(row):
        return pltpu.make_async_copy(buf.at[row], out.at[row], sem.at[row])

    def face(c, first):
        use_one = y_odd if first else jnp.logical_not(y_odd)
        at = pl.ds(96 + 16 * c, 16)
        own = jnp.where(use_one, got1[at, :], got3[at, :])
        at = pl.ds(144 + 16 * c, 16)
        sent = jnp.where(use_one, got1[at, :], got3[at, :])
        at = pl.ds(16 * c, 16)
        of_lo = jnp.where(x_odd, near[at, :], far[at, :])
        of_hi = jnp.where(x_odd, far[at, :], near[at, :])
        if first:
            got = jnp.where(low_slots, of_lo, pltpu.roll(of_hi, 32, 1))
        else:
            got = jnp.where(low_slots, pltpu.roll(of_lo, 96, 1), of_hi)
        total = own + jnp.where(here, got, 0.0)
        new = jnp.where((lane < 8) & has_before, got + pltpu.roll(sent, 40, 1), total)
        new = jnp.where((lane >= 120) & has_after, got + pltpu.roll(sent, 88, 1), new)
        new = jnp.where((lane >= 88) & (lane < 96), total + pltpu.roll(total, 56, 1), new)
        new = jnp.where((lane >= 32) & (lane < 40), total + pltpu.roll(total, 72, 1), new)
        return jnp.where(gy > 0 if first else gy < N_GY - 1, new, 0.0)

    last_passes(
        field,
        (0, 3),
        lambda c: face(c, True),
        lambda c: face(c, False),
        buf,
        lambda row: copy(row).start(),
    )
    for row in range(24):
        if row % 4 in (0, 3):
            copy(row).wait()


def swapped(x, axis, partner):
    return lax.ppermute(x, axis, [(i, partner(i)) for i in range(lax.axis_size(axis))])


def body(velocity, part_pos, part_vel, part_coef, counts, dest, elem):
    pos = part_pos.transpose(1, 0, 2)
    vel = part_vel.transpose(1, 0, 2)
    coef = part_coef.reshape(256, 128)
    nodes = jnp.asarray(node_table())
    send, block, own_elem = call(
        pack_kernel,
        [((N_GY * ROWS, 128), F32, "vmem"), ((128,), jnp.int32, "smem"), ((128,), jnp.int32, "smem")],
        [(a, "raw") for a in (dest, counts, elem, pos, vel, coef)],
        (SMEM((128,), jnp.int32),) * 3
        + (VMEM(pos.shape, F32),) * 2
        + (VMEM(coef.shape, F32), pltpu.SemaphoreType.DMA((9,))),
    )
    own = send[:ROWS]
    groups = {
        k: swapped(send[k * ROWS : (k + 1) * ROWS], "gy", lambda i, k=k: i ^ k) for k in ORDER
    }
    field, parts, drag_own, table = call(
        own_kernel,
        [((8 * 24 * PITCH, 128), F32, "vmem"), ((8 * 36 * PITCH, 128), F32, "vmem"), ((96, 128), F32, "vmem"), (nodes.shape, F32, "vmem")],
        [(own_elem, "smem"), (own, "vmem"), (velocity.reshape(24, 16, 512), "hbm"), (nodes, "hbm")],
        (VMEM((96, 128), F32),),
        flops=OWN_FLOPS,
    )
    grid = (24, 16, 512)
    send3, send1, drag2, inside, ghosts, _ = call(
        rest_kernel,
        [((192, 128), F32, "vmem")] * 2
        + [((96, 128), F32, "vmem")]
        + [(grid, F32, "vmem")] * 2
        + [((8 * 36 * PITCH, 128), F32, "vmem")],
        [(groups[k], "vmem") for k in ORDER]
        + [(field, "vmem"), (table, "vmem"), (parts, "vmem")],
        (
            VMEM((96, 128), F32),
            VMEM((8, 128), jnp.int32),
            SMEM((8, 128), jnp.int32),
            pltpu.SemaphoreType.DMA,
        ),
        aliases={5: 5},
    )
    last_gx = lax.axis_size("gx") - 1

    def to_far(i):
        other = i + 1 if i & 1 else i - 1
        return other if 0 <= other <= last_gx else i

    far = swapped(ghosts[12:], "gx", to_far)
    near = swapped(ghosts[:12], "gx", lambda i: i ^ 1)
    got1 = swapped(send1, "gy", lambda i: i ^ 1)
    got3 = swapped(send3, "gy", lambda i: i ^ 3)
    back2 = swapped(drag2, "gy", lambda i: i ^ 2)
    forward_near, forward_far = call(
        forward_kernel,
        [((48, 128), F32, "vmem")] * 2,
        [(got1, "vmem"), (got3, "vmem")],
    )
    got_far = swapped(forward_far, "gx", to_far)
    got_near = swapped(forward_near, "gx", lambda i: i ^ 1)
    drag, out, field = call(
        lambda *refs: inner_kernel(last_gx, *refs),
        [((384, 128), F32, "raw"), (grid, F32, "raw"), (grid, F32, "vmem")],
        [(block, "smem")]
        + [(a, "vmem") for a in (inside, ghosts, near, far, drag_own, got1, back2, got3)],
        (
            VMEM((384, 128), F32),
            VMEM(grid, F32),
            pltpu.SemaphoreType.DMA((24,)),
            pltpu.SemaphoreType.DMA((4,)),
        ),
        flops=INNER_FLOPS,
    )
    (out,) = call(
        lambda *refs: outer_kernel(last_gx, *refs),
        [(grid, F32, "raw")],
        [(a, "vmem") for a in (field, got1, got3, got_near, got_far)] + [(out, "raw")],
        (VMEM(grid, F32), pltpu.SemaphoreType.DMA((24,))),
        aliases={5: 0},
    )
    return (
        drag.reshape(3, 128, 128).transpose(1, 0, 2),
        out.reshape(velocity.shape),
    )


def solution(mesh):
    in_specs = (
        P(None, "gx", "gy", None, None),
        P(("gx", "gy"), None, None),
        P(("gx", "gy"), None, None),
        P(("gx", "gy"), None, None),
        P(("gx", "gy")),
        P(("gx", "gy")),
        P(("gx", "gy")),
    )
    out_specs = (P(("gx", "gy"), None, None), P(None, "gx", "gy", None, None))
    return jax.shard_map(body, mesh=mesh, in_specs=in_specs, out_specs=out_specs, check_vma=False)
```

```python
import jax
import jax.numpy as jnp
import numpy as np
from jax import lax
from jax.experimental import pallas as pl
from jax.experimental.pallas import tpu as pltpu
from jax.sharding import PartitionSpec as P

GLL = (
    -1.0,
    -0.8717401485096066,
    -0.5917001814331423,
    -0.2092992179024789,
    0.2092992179024789,
    0.5917001814331423,
    0.8717401485096066,
    1.0,
)
SHARPNESS = 8.0
INTERPRET = False
F32 = jnp.float32
BF16 = jnp.bfloat16
VMEM = pltpu.VMEM
SMEM = pltpu.SMEM
N_GY = 4
SHARE = 32
ROWS = 264
PAIRED = (0, 2, 4, 6, 1, 3, 5, 7)


def node_table():
    q = np.array(GLL, np.float64)
    rows = []
    for order in (tuple(range(8)), PAIRED):
        for t in range(7):
            rows.append([q[[m for m in range(8) if m != i][t]] for i in order])
        rows.append([1.0 / np.prod([q[i] - q[m] for m in range(8) if m != i]) for i in order])
    rows.append([q[i] for i in range(8)])
    for first, second in ((-2.0, 0.0), (2.0, 2.0)):
        for half in (PAIRED[:4], PAIRED[4:]):
            rows.append([q[i] + first for i in half] + [q[i] + second for i in half])
    table = np.array(rows, np.float32).reshape(-1, 1)
    return np.ascontiguousarray(np.broadcast_to(table, (table.shape[0], 128)))


PITCH = 17
ORDER = (3, 1, 2)
UNROLL_A = 32
UNROLL_B = 32
OWN_FLOPS = 2_000_000_000
UNPACK_FLOPS = 1_000_000_000


SPACES = {"vmem": VMEM, "hbm": VMEM, "": VMEM, "smem": SMEM, "table": SMEM, "raw": pltpu.HBM}


def call(kernel, outs, ins, scratch=(), flops=0, aliases=None):
    args = [
        a
        if INTERPRET
        else pltpu.with_memory_space_constraint(a, VMEM if m == "vmem" else pltpu.HBM)
        if m in ("vmem", "hbm", "table", "raw")
        else a
        for a, m in ins
    ]
    shapes = [
        VMEM(shape, dtype) if m == "vmem" and not INTERPRET else jax.ShapeDtypeStruct(shape, dtype)
        for shape, dtype, m in outs
    ]
    return pl.pallas_call(
        kernel,
        out_shape=shapes,
        in_specs=[pl.BlockSpec(memory_space=SPACES[m]) for _, m in ins],
        out_specs=[pl.BlockSpec(memory_space=SPACES[m]) for _, _, m in outs],
        scratch_shapes=scratch,
        interpret=INTERPRET,
        input_output_aliases=aliases or {},
        compiler_params=pltpu.CompilerParams(vmem_limit_bytes=24 * 1024 * 1024),
        cost_estimate=pl.CostEstimate(flops=flops, bytes_accessed=0, transcendentals=0),
    )(*args)


def lanes(shape=(1, 128)):
    return lax.broadcasted_iota(jnp.int32, shape, len(shape) - 1)


def pack_kernel(
    dest_hbm, counts_hbm, elem_hbm, pos_hbm, vel_hbm, coef_hbm,
    send, block, own_elem,
    dest, counts, elem, pos, vel, coef, sem,
):
    tables = [
        pltpu.make_async_copy(a, b, sem.at[k])
        for k, (a, b) in enumerate(((dest_hbm, dest), (counts_hbm, counts), (elem_hbm, elem)))
    ]
    halves = []
    for k in range(2):
        cut = pl.ds(64 * k, 64)
        pairs = (
            (pos_hbm.at[:, cut], pos.at[:, cut]),
            (vel_hbm.at[:, cut], vel.at[:, cut]),
            (coef_hbm.at[pl.ds(128 * k, 128)], coef.at[pl.ds(128 * k, 128)]),
        )
        halves.append(
            [pltpu.make_async_copy(a, b, sem.at[3 + 3 * k + n]) for n, (a, b) in enumerate(pairs)]
        )
    for copy in tables + halves[0] + halves[1]:
        copy.start()
    me = lax.axis_index("gy")
    lane = lanes()
    ids = lax.broadcasted_iota(jnp.int32, (8, 128), 0) * 128 + lanes((8, 128))

    def one(b, state):
        taken, labels = state
        d = dest[b] ^ me
        r = (taken >> (8 * d)) & 255
        e = elem[b]
        block[d * SHARE + r] = b
        own_elem[d * SHARE + r] = e
        base = d * ROWS + r
        send[pl.ds(base, 3, stride=32), :] = pos[:, b, :]
        send[pl.ds(base + 96, 3, stride=32), :] = vel[:, b, :]
        rate = coef[pl.ds(2 * b, 1), :]
        send[pl.ds(base + 192, 1), :] = jnp.where(lane < counts[b], rate, 0.0)
        send[pl.ds(base + 224, 1), :] = coef[pl.ds(2 * b + 1, 1), :]
        labels = jnp.where(ids == d * 128 + r, e, labels)
        return (taken + (1 << (8 * d)), labels)

    state = (jnp.int32(0), jnp.zeros((8, 128), jnp.int32))
    for copy in tables:
        copy.wait()
    for k in range(2):
        for copy in halves[k]:
            copy.wait()
        state = lax.fori_loop(64 * k, 64 * k + 64, one, state, unroll=8)
    labels = state[1].astype(F32)
    for d in range(N_GY):
        send[d * ROWS + 256 : d * ROWS + 264, :] = jnp.broadcast_to(labels[d : d + 1, :], (8, 128))


def split_two(x):
    high = x.astype(BF16)
    low = (x - high.astype(F32)).astype(BF16)
    return high, low


def lagrange(x, nodes, first):
    out = nodes[8 * (first + 7) : 8 * (first + 8), :]
    for t in range(7):
        out = out * (x - nodes[8 * (first + t) : 8 * (first + t + 1), :])
    return out


def gauss(x, nodes, row):
    d = nodes[8 * row : 8 * row + 8, :] - x
    return jnp.exp(d * d * (-SHARPNESS))


def outer(a, b):
    return jnp.concatenate([a[j : j + 1, :] * b for j in range(8)], axis=0)


def spread_field(vel, field):
    low_half = lanes() < 64

    def one(xy, _):
        for c in range(3):
            for h in range(4):
                t = vel[c * 8 + xy, :, 128 * h : 128 * h + 128].astype(F32)
                turned = pltpu.roll(t, 64, 1)
                at = (xy * 24 + c * 8 + h) * PITCH
                field[pl.ds(at, 16), :] = jnp.where(low_half, t, turned)
                field[pl.ds(at + 4 * PITCH, 16), :] = jnp.where(low_half, turned, t)
        return 0

    lax.fori_loop(0, 8, one, 0)


def interpolate(group, element, field, nodes, fluid):
    def one(r, _):
        e = element(r)
        basis_r = lagrange(group[pl.ds(r, 1), :], nodes, 8)
        basis_s = lagrange(group[pl.ds(r + 32, 1), :], nodes, 0)
        basis_t = lagrange(group[pl.ds(r + 64, 1), :], nodes, 0)
        high, low = split_two(outer(basis_s, basis_t))
        nodal = field[pl.ds((e >> 4) * (24 * PITCH) + (e & 15), 24, stride=PITCH), :].astype(BF16)
        part = jnp.dot(nodal, jnp.concatenate([high, low], axis=0), preferred_element_type=F32)
        for c in range(3):
            fluid[pl.ds(c * 32 + r, 1), :] = jnp.sum(
                part[8 * c : 8 * c + 8, :] * basis_r, axis=0, keepdims=True
            )
        return 0

    lax.fori_loop(0, SHARE, one, 0, unroll=UNROLL_A)


def find_drag(group, fluid, drag):
    w = [
        fluid[32 * c : 32 * c + 32, :] - group[96 + 32 * c : 128 + 32 * c, :] for c in range(3)
    ]
    scale = group[224:256, :]
    square = (w[0] * w[0] + w[1] * w[1] + w[2] * w[2]) * (scale * scale)
    power = jnp.where(square > 0.0, jnp.exp(0.3435 * jnp.log(square)), 0.0)
    factor = group[192:224, :] * (1.0 + 0.15 * power)
    for c in range(3):
        drag[32 * c : 32 * c + 32, :] = factor * w[c]


def project(group, element, drag, nodes, parts):
    low_half = lanes() < 64
    upper_rows = lax.broadcasted_iota(jnp.int32, (8, 128), 0) < 4

    def one(r, _):
        e = element(r)
        x = group[pl.ds(r, 1), :]
        near = [gauss(x, nodes, 17 + k) for k in range(2)]
        after = [gauss(x, nodes, 19 + k) for k in range(2)]
        planes = outer(
            gauss(group[pl.ds(r + 32, 1), :], nodes, 16),
            gauss(group[pl.ds(r + 64, 1), :], nodes, 16),
        )
        planes = jnp.concatenate(split_two(planes), axis=0)
        force = [-drag[pl.ds(c * 32 + r, 1), :] for c in range(3)]
        mixed = jnp.where(upper_rows, force[0], force[1])
        rows = []
        for k in range(2):
            rows += [near[k] * f for f in force] + [after[k] * mixed, after[k] * force[2]]
        rows = jnp.concatenate(split_two(jnp.concatenate(rows, axis=0)), axis=0)
        both = lax.dot_general(
            rows, planes, (((1,), (1,)), ((), ())), preferred_element_type=F32
        )
        both = both[:80, :] + both[80:, :]
        at = (e >> 4) * (36 * PITCH) + (e & 15)
        for k in range(5):
            even = both[8 * k : 8 * k + 8, :]
            odd = both[40 + 8 * k : 48 + 8 * k, :]
            t = jnp.where(low_half, even, odd)
            t = t + pltpu.roll(jnp.where(low_half, odd, even), 64, 1)
            n = 8 if k < 4 else 4
            parts[pl.ds(at + k * 8 * PITCH, n, stride=PITCH), :] = t[0:n, :]
        return 0

    lax.fori_loop(0, SHARE, one, 0, unroll=UNROLL_B)


def own_kernel(elem, group, vel, nodes, field, parts, drag, table, fluid):
    def element(r):
        return elem[r]

    table[...] = nodes[...]
    spread_field(vel, field)
    interpolate(group, element, field, nodes, fluid)
    find_drag(group, fluid, drag)
    project(group, element, drag, nodes, parts)


def fetch_elements(groups, lab_v, lab_s, sem):
    for k, g in enumerate(groups):
        lab_v[k : k + 1, :] = g[256:257, :].astype(jnp.int32)
    copy = pltpu.make_async_copy(lab_v, lab_s, sem)
    copy.start()
    copy.wait()
    return [lambda r, k=k: lab_s[k, r] for k in range(len(groups))]


def middle_kernel(group, field, nodes, _, drag, parts, fluid, lab_v, lab_s, sem):
    (element,) = fetch_elements((group,), lab_v, lab_s, sem)
    interpolate(group, element, field, nodes, fluid)
    find_drag(group, fluid, drag)
    project(group, element, drag, nodes, parts)


def rest_kernel(ga, gb, field, nodes, _, da, db, inside, ghosts, parts, fluid, lab_v, lab_s, sem):
    groups = (ga, gb)
    drags = (da, db)
    elements = fetch_elements(groups, lab_v, lab_s, sem)
    for k in range(2):
        interpolate(groups[k], elements[k], field, nodes, fluid)
        find_drag(groups[k], fluid, drags[k])
    for k in range(2):
        project(groups[k], elements[k], drags[k], nodes, parts)
    gather_parts(parts, inside, ghosts)


def gather_parts(parts, inside, ghosts):
    low_half = lanes() < 64
    odd = lax.axis_index("gx") & 1
    to_lo = (1 - odd) * 12
    to_hi = odd * 12

    def part(x, y, c, k, h):
        n = 2 * c + k if k < 2 else 6 + c
        return parts[pl.ds(((x * 4 + y) * 36 + n * 4 + h) * PITCH, 16), :]

    def one(y, _):
        for c in range(3):
            lower = []
            upper = []
            for h in range(4):
                lo = part(0, y, c, 1, h) + part(1, y, c, 0, h)
                hi = part(1, y, c, 1, h) + part(0, y, c, 2, h)
                inside[c * 8 + y, :, 128 * h : 128 * h + 128] = lo
                inside[c * 8 + 4 + y, :, 128 * h : 128 * h + 128] = hi
                lower.append(lo)
                upper.append(hi)
            for h in range(4):
                lo = part(0, y, c, 0, h)
                hi = part(1, y, c, 2, h)
                if h == 3:
                    lo = lo + jnp.where(low_half, 0.0, pltpu.roll(lower[0], 64, 1))
                if h == 0:
                    hi = hi + jnp.where(low_half, pltpu.roll(upper[3], 64, 1), 0.0)
                ghosts[to_lo + c * 4 + y, :, 128 * h : 128 * h + 128] = lo
                ghosts[to_hi + c * 4 + y, :, 128 * h : 128 * h + 128] = hi
        return 0

    lax.fori_loop(0, 4, one, 0)


def first_pass_kernel(last_gx, inside, sent, near, far, field, faces):
    low_half = lanes() < 64
    spot = (lanes() % 64) // 8
    gx = lax.axis_index("gx")
    odd = (gx & 1) == 1
    has_before = gx > 0
    has_after = gx < last_gx
    to_lo = (1 - (gx & 1)) * 12
    to_hi = (gx & 1) * 12
    y_odd = (lax.axis_index("gy") & 1) == 1

    def cut(ref, at, h):
        return ref[at, :, 128 * h : 128 * h + 128]

    for c in range(3):
        packed = [jnp.zeros((16, 128), F32), jnp.zeros((16, 128), F32)]
        for y in range(4):
            pair = [(cut(near, c * 4 + y, h), cut(far, c * 4 + y, h)) for h in range(4)]
            got_lo = [jnp.where(odd, n, f) for n, f in pair]
            got_hi = [jnp.where(odd, f, n) for n, f in pair]
            lower = [
                cut(inside, c * 8 + y, h) + jnp.where(has_before, got_lo[h], 0.0) for h in range(4)
            ]
            upper = [
                cut(inside, c * 8 + 4 + y, h) + jnp.where(has_after, got_hi[h], 0.0)
                for h in range(4)
            ]
            first = got_lo[0] + pltpu.roll(cut(sent, to_lo + c * 4 + y, 3), 64, 1)
            last = got_hi[3] + pltpu.roll(cut(sent, to_hi + c * 4 + y, 0), 64, 1)
            low3, up0 = lower[3], upper[0]
            lower[0] = jnp.where(low_half & has_before, first, lower[0])
            upper[3] = jnp.where(low_half | jnp.logical_not(has_after), upper[3], last)
            lower[3] = jnp.where(low_half, low3, low3 + pltpu.roll(up0, 64, 1))
            upper[0] = jnp.where(low_half, up0 + pltpu.roll(low3, 64, 1), up0)
            for x, layer in ((0, lower), (1, upper)):
                for h in range(4):
                    field[c * 8 + x * 4 + y, :, 128 * h : 128 * h + 128] = layer[h]
                    k = x * 4 + h
                    if y == 0:
                        moved = pltpu.roll(layer[h], 8 * k, 1) if k else layer[h]
                        packed[0] = jnp.where(spot == k, moved, packed[0])
                    if y == 3:
                        by = (8 * k - 56) % 128
                        moved = pltpu.roll(layer[h], by, 1) if by else layer[h]
                        packed[1] = jnp.where(spot == k, moved, packed[1])
        faces[16 * c : 16 * c + 16, :] = jnp.where(y_odd, packed[0], packed[1])
        faces[48 + 16 * c : 64 + 16 * c, :] = jnp.where(y_odd, packed[1], packed[0])


def last_passes(field, rows, before, after, buf, start):
    lane = lanes()
    bottom = (lane % 64) < 8
    top = (lane % 64) >= 56
    z = lax.broadcasted_iota(jnp.int32, (16, 128), 0)
    lane16 = lanes((16, 128))
    up_here = (lane16 % 8 == 7) & (z < 15)
    down_here = (lane16 % 8 == 0) & (z > 0)

    def one_comp(c, _):
        lo_pack = before(c)
        hi_pack = after(c)
        for x in range(2):
            for y in rows:
                for h in range(4):
                    k = x * 4 + h

                    def at(row):
                        return field[c * 8 + x * 4 + row, :, 128 * h : 128 * h + 128]

                    if y == 3:
                        above = hi_pack if k == 7 else pltpu.roll(hi_pack, 56 - 8 * k, 1)
                    else:
                        above = pltpu.roll(at(y + 1), 56, 1)
                    if y == 0:
                        below = lo_pack if k == 0 else pltpu.roll(lo_pack, 128 - 8 * k, 1)
                    else:
                        below = pltpu.roll(at(y - 1), 72, 1)
                    g = at(y) + jnp.where(top, above, jnp.where(bottom, below, 0.0))
                    above = pltpu.roll(pltpu.roll(g, 7, 1), 15, 0)
                    below = pltpu.roll(pltpu.roll(g, 121, 1), 1, 0)
                    g = g + jnp.where(up_here, above, jnp.where(down_here, below, 0.0))
                    buf[c * 8 + x * 4 + y, :, 128 * h : 128 * h + 128] = g
                start(c * 8 + x * 4 + y)
        return 0

    lax.fori_loop(0, 3, one_comp, 0)


def inner_kernel(block, field, d0, d1, d2, d3, drag, out):
    for k, d in enumerate((d0, d1, d2, d3)):

        def one(r, _):
            drag[pl.ds(block[k * SHARE + r], 3, stride=128), :] = d[pl.ds(r, 3, stride=32), :]
            return 0

        lax.fori_loop(0, SHARE, one, 0, unroll=8)
    last_passes(field, (1, 2), lambda c: None, lambda c: None, out, lambda row: None)


def outer_kernel(field, got1, got3, done, drag_done, drag, out, buf, sem, drag_sem):
    gy = lax.axis_index("gy")
    odd = (gy & 1) == 1
    between = (gy > 0) & (gy < N_GY - 1)
    moves = [
        pltpu.make_async_copy(
            drag_done.at[pl.ds(96 * k, 96)], drag.at[pl.ds(96 * k, 96)], drag_sem.at[k]
        )
        for k in range(4)
    ] + [
        pltpu.make_async_copy(done.at[row], out.at[row], sem.at[row])
        for row in range(24)
        if row % 4 in (1, 2)
    ]
    for move in moves:
        move.start()

    def copy(row):
        return pltpu.make_async_copy(buf.at[row], out.at[row], sem.at[row])

    def face(c, first):
        a = got1[pl.ds(16 * c, 16), :]
        b = jnp.where(between, got3[pl.ds(16 * c, 16), :], 0.0)
        return jnp.where(odd, a, b) if first else jnp.where(odd, b, a)

    last_passes(
        field,
        (0, 3),
        lambda c: face(c, True),
        lambda c: face(c, False),
        buf,
        lambda row: copy(row).start(),
    )
    for move in moves:
        move.wait()
    for row in range(24):
        if row % 4 in (0, 3):
            copy(row).wait()


def swapped(x, axis, partner):
    return lax.ppermute(x, axis, [(i, partner(i)) for i in range(lax.axis_size(axis))])


def swapped_all(x, partner):
    nx, ny = lax.axis_size("gx"), lax.axis_size("gy")
    pairs = []
    for i in range(nx):
        for j in range(ny):
            a, b = partner(i, j)
            pairs.append((i * ny + j, a * ny + b))
    return lax.ppermute(x, ("gx", "gy"), pairs)


def body(velocity, part_pos, part_vel, part_coef, counts, dest, elem):
    pos = part_pos.transpose(1, 0, 2)
    vel = part_vel.transpose(1, 0, 2)
    coef = part_coef.reshape(256, 128)
    nodes = jnp.asarray(node_table())
    send, block, own_elem = call(
        pack_kernel,
        [((N_GY * ROWS, 128), F32, "vmem"), ((128,), jnp.int32, "smem"), ((128,), jnp.int32, "smem")],
        [(a, "raw") for a in (dest, counts, elem, pos, vel, coef)],
        (SMEM((128,), jnp.int32),) * 3
        + (VMEM(pos.shape, F32),) * 2
        + (VMEM(coef.shape, F32), pltpu.SemaphoreType.DMA((9,))),
    )
    own = send[:ROWS]
    groups = {
        k: swapped(send[k * ROWS : (k + 1) * ROWS], "gy", lambda i, k=k: i ^ k) for k in ORDER
    }
    field, parts, drag_own, table = call(
        own_kernel,
        [((8 * 24 * PITCH, 128), F32, "vmem"), ((8 * 36 * PITCH, 128), F32, "vmem"), ((96, 128), F32, "vmem"), (nodes.shape, F32, "vmem")],
        [(own_elem, "smem"), (own, "vmem"), (velocity.reshape(24, 16, 512), "hbm"), (nodes, "hbm")],
        (VMEM((96, 128), F32),),
        flops=OWN_FLOPS,
    )
    labels = (
        VMEM((96, 128), F32),
        VMEM((8, 128), jnp.int32),
        SMEM((8, 128), jnp.int32),
        pltpu.SemaphoreType.DMA,
    )
    first, *others = reversed(ORDER)
    drags = {}
    drags[first], parts = call(
        middle_kernel,
        [((96, 128), F32, "vmem"), ((8 * 36 * PITCH, 128), F32, "vmem")],
        [(a, "vmem") for a in (groups[first], field, table, parts)],
        labels,
        flops=OWN_FLOPS,
        aliases={3: 1},
    )
    drags[others[1]], drags[others[0]], inside, ghosts, _ = call(
        rest_kernel,
        [((96, 128), F32, "vmem")] * 2
        + [((24, 16, 512), F32, "vmem")] * 2
        + [((8 * 36 * PITCH, 128), F32, "vmem")],
        [(a, "vmem") for a in (groups[others[1]], groups[others[0]], field, table, parts)],
        labels,
        aliases={4: 4},
    )
    last_gx = lax.axis_size("gx") - 1

    def other_chip(i, j):
        k = i + 1 if i & 1 else i - 1
        return (k, j) if 0 <= k <= last_gx else (i, j ^ 1)

    far = swapped_all(ghosts[12:], other_chip)
    near = swapped(ghosts[:12], "gx", lambda i: i ^ 1)
    back = {k: swapped(d, "gy", lambda i, k=k: i ^ k) for k, d in drags.items()}
    last_gx = lax.axis_size("gx") - 1
    field, faces = call(
        lambda *refs: first_pass_kernel(last_gx, *refs),
        [((24, 16, 512), F32, "vmem"), ((96, 128), F32, "vmem")],
        [(inside, "vmem"), (ghosts, "vmem"), (near, "vmem"), (far, "vmem")],
    )
    got1 = swapped(faces[:48], "gy", lambda i: i ^ 1)
    got3 = swapped_all(faces[48:], lambda i, j: (i, j ^ 3) if 0 < j < N_GY - 1 else (i ^ 1, j))
    grid = (24, 16, 512)
    drag, inner = call(
        inner_kernel,
        [((384, 128), F32, "vmem"), (grid, F32, "vmem")],
        [(block, "smem"), (field, "vmem"), (drag_own, "vmem")]
        + [(back[k], "vmem") for k in range(1, N_GY)],
        flops=UNPACK_FLOPS,
    )
    drag, out = call(
        outer_kernel,
        [((384, 128), F32, "raw"), (grid, F32, "raw")],
        [(a, "vmem") for a in (field, got1, got3, inner, drag)],
        (VMEM(grid, F32), pltpu.SemaphoreType.DMA((24,)), pltpu.SemaphoreType.DMA((4,))),
    )
    return (
        drag.reshape(3, 128, 128).transpose(1, 0, 2),
        out.reshape(velocity.shape),
    )


def solution(mesh):
    in_specs = (
        P(None, "gx", "gy", None, None),
        P(("gx", "gy"), None, None),
        P(("gx", "gy"), None, None),
        P(("gx", "gy"), None, None),
        P(("gx", "gy")),
        P(("gx", "gy")),
        P(("gx", "gy")),
    )
    out_specs = (P(("gx", "gy"), None, None), P(None, "gx", "gy", None, None))
    return jax.shard_map(body, mesh=mesh, in_specs=in_specs, out_specs=out_specs, check_vma=False)
```

```python
import jax
import jax.numpy as jnp
import numpy as np
from jax import lax
from jax.experimental import pallas as pl
from jax.experimental.pallas import tpu as pltpu
from jax.sharding import PartitionSpec as P

GLL = (
    -1.0,
    -0.8717401485096066,
    -0.5917001814331423,
    -0.2092992179024789,
    0.2092992179024789,
    0.5917001814331423,
    0.8717401485096066,
    1.0,
)
SHARPNESS = 8.0
INTERPRET = False
F32 = jnp.float32
BF16 = jnp.bfloat16
VMEM = pltpu.VMEM
SMEM = pltpu.SMEM
N_GY = 4
SHARE = 32
ROWS = 264
PAIRED = (0, 2, 4, 6, 1, 3, 5, 7)


def node_table():
    q = np.array(GLL, np.float64)
    rows = []
    for order in (tuple(range(8)), PAIRED):
        for t in range(7):
            rows.append([q[[m for m in range(8) if m != i][t]] for i in order])
        rows.append([1.0 / np.prod([q[i] - q[m] for m in range(8) if m != i]) for i in order])
    rows.append([q[i] for i in range(8)])
    for first, second in ((-2.0, 0.0), (2.0, 2.0)):
        for half in (PAIRED[:4], PAIRED[4:]):
            rows.append([q[i] + first for i in half] + [q[i] + second for i in half])
    table = np.array(rows, np.float32).reshape(-1, 1)
    return np.ascontiguousarray(np.broadcast_to(table, (table.shape[0], 128)))


PITCH = 17
ORDER = (2, 1, 3)
OWN_FLOPS = 2_000_000_000
UNPACK_FLOPS = 1_000_000_000


SPACES = {"vmem": VMEM, "hbm": VMEM, "": VMEM, "smem": SMEM, "table": SMEM, "raw": pltpu.HBM}


def call(kernel, outs, ins, scratch=(), flops=0, aliases=None):
    args = [
        a
        if INTERPRET
        else pltpu.with_memory_space_constraint(a, VMEM if m == "vmem" else pltpu.HBM)
        if m in ("vmem", "hbm", "table", "raw")
        else a
        for a, m in ins
    ]
    shapes = [
        VMEM(shape, dtype) if m == "vmem" and not INTERPRET else jax.ShapeDtypeStruct(shape, dtype)
        for shape, dtype, m in outs
    ]
    return pl.pallas_call(
        kernel,
        out_shape=shapes,
        in_specs=[pl.BlockSpec(memory_space=SPACES[m]) for _, m in ins],
        out_specs=[pl.BlockSpec(memory_space=SPACES[m]) for _, _, m in outs],
        scratch_shapes=scratch,
        interpret=INTERPRET,
        input_output_aliases=aliases or {},
        compiler_params=pltpu.CompilerParams(vmem_limit_bytes=24 * 1024 * 1024),
        cost_estimate=pl.CostEstimate(flops=flops, bytes_accessed=0, transcendentals=0),
    )(*args)


def lanes(shape=(1, 128)):
    return lax.broadcasted_iota(jnp.int32, shape, len(shape) - 1)


def pack_kernel(
    dest_hbm, counts_hbm, elem_hbm, pos_hbm, vel_hbm, coef_hbm, velocity_hbm,
    send, block, own_elem, velocity,
    dest, counts, elem, pos, vel, coef, sem,
):
    tables = [
        pltpu.make_async_copy(a, b, sem.at[k])
        for k, (a, b) in enumerate(((dest_hbm, dest), (counts_hbm, counts), (elem_hbm, elem)))
    ]
    halves = []
    for k in range(2):
        cut = pl.ds(64 * k, 64)
        pairs = (
            (pos_hbm.at[:, cut], pos.at[:, cut]),
            (vel_hbm.at[:, cut], vel.at[:, cut]),
            (coef_hbm.at[pl.ds(128 * k, 128)], coef.at[pl.ds(128 * k, 128)]),
        )
        halves.append(
            [pltpu.make_async_copy(a, b, sem.at[3 + 3 * k + n]) for n, (a, b) in enumerate(pairs)]
        )
    fetch = pltpu.make_async_copy(velocity_hbm, velocity, sem.at[9])
    for copy in tables + halves[0] + halves[1] + [fetch]:
        copy.start()
    me = lax.axis_index("gy")
    lane = lanes()
    ids = lax.broadcasted_iota(jnp.int32, (8, 128), 0) * 128 + lanes((8, 128))

    def one(b, state):
        taken, labels = state
        d = dest[b] ^ me
        r = (taken >> (8 * d)) & 255
        e = elem[b]
        block[d * SHARE + r] = b
        own_elem[d * SHARE + r] = e
        base = d * ROWS + r
        send[pl.ds(base, 3, stride=32), :] = pos[:, b, :]
        send[pl.ds(base + 96, 3, stride=32), :] = vel[:, b, :]
        rate = coef[pl.ds(2 * b, 1), :]
        send[pl.ds(base + 192, 1), :] = jnp.where(lane < counts[b], rate, 0.0)
        send[pl.ds(base + 224, 1), :] = coef[pl.ds(2 * b + 1, 1), :]
        labels = jnp.where(ids == d * 128 + r, e, labels)
        return (taken + (1 << (8 * d)), labels)

    state = (jnp.int32(0), jnp.zeros((8, 128), jnp.int32))
    for copy in tables:
        copy.wait()
    for k in range(2):
        for copy in halves[k]:
            copy.wait()
        state = lax.fori_loop(64 * k, 64 * k + 64, one, state, unroll=8)
    fetch.wait()
    labels = state[1].astype(F32)
    for d in range(N_GY):
        send[d * ROWS + 256 : d * ROWS + 264, :] = jnp.broadcast_to(labels[d : d + 1, :], (8, 128))


def split_two(x):
    high = x.astype(BF16)
    low = (x - high.astype(F32)).astype(BF16)
    return high, low


def lagrange(x, nodes, first):
    out = nodes[8 * (first + 7) : 8 * (first + 8), :]
    for t in range(7):
        out = out * (x - nodes[8 * (first + t) : 8 * (first + t + 1), :])
    return out


def gauss(x, nodes, row):
    d = nodes[8 * row : 8 * row + 8, :] - x
    return jnp.exp(d * d * (-SHARPNESS))


def outer(a, b):
    return jnp.concatenate([a[j : j + 1, :] * b for j in range(8)], axis=0)


def spread_field(vel, field):
    low_half = lanes() < 64

    def one(xy, _):
        for c in range(3):
            for h in range(4):
                t = vel[c * 8 + xy, :, 128 * h : 128 * h + 128].astype(F32)
                turned = pltpu.roll(t, 64, 1)
                at = (xy * 24 + c * 8 + h) * PITCH
                field[pl.ds(at, 16), :] = jnp.where(low_half, t, turned)
                field[pl.ds(at + 4 * PITCH, 16), :] = jnp.where(low_half, turned, t)
        return 0

    lax.fori_loop(0, 8, one, 0)


def interpolate(group, elements, field, nodes, fluid):
    for r in range(SHARE):
        e = elements[r]
        basis_r = lagrange(group[r : r + 1, :], nodes, 8)
        basis_s = lagrange(group[r + 32 : r + 33, :], nodes, 0)
        basis_t = lagrange(group[r + 64 : r + 65, :], nodes, 0)
        high, low = split_two(outer(basis_s, basis_t))
        nodal = field[pl.ds((e >> 4) * (24 * PITCH) + (e & 15), 24, stride=PITCH), :].astype(BF16)
        part = jnp.dot(nodal, jnp.concatenate([high, low], axis=0), preferred_element_type=F32)
        for c in range(3):
            fluid[c * 32 + r : c * 32 + r + 1, :] = jnp.sum(
                part[8 * c : 8 * c + 8, :] * basis_r, axis=0, keepdims=True
            )


def find_drag(group, fluid, drag):
    w = [
        fluid[32 * c : 32 * c + 32, :] - group[96 + 32 * c : 128 + 32 * c, :] for c in range(3)
    ]
    scale = group[224:256, :]
    square = (w[0] * w[0] + w[1] * w[1] + w[2] * w[2]) * (scale * scale)
    power = jnp.where(square > 0.0, jnp.exp(0.3435 * jnp.log(square)), 0.0)
    factor = group[192:224, :] * (1.0 + 0.15 * power)
    for c in range(3):
        drag[32 * c : 32 * c + 32, :] = factor * w[c]


def project(group, elements, drag, nodes, parts):
    low_half = lanes() < 64
    upper_rows = lax.broadcasted_iota(jnp.int32, (8, 128), 0) < 4

    for r in range(SHARE):
        e = elements[r]
        x = group[r : r + 1, :]
        near = [gauss(x, nodes, 17 + k) for k in range(2)]
        after = [gauss(x, nodes, 19 + k) for k in range(2)]
        planes = outer(
            gauss(group[r + 32 : r + 33, :], nodes, 16),
            gauss(group[r + 64 : r + 65, :], nodes, 16),
        )
        planes = jnp.concatenate(split_two(planes), axis=0)
        force = [-drag[c * 32 + r : c * 32 + r + 1, :] for c in range(3)]
        mixed = jnp.where(upper_rows, force[0], force[1])
        rows = []
        for k in range(2):
            rows += [near[k] * f for f in force] + [after[k] * mixed, after[k] * force[2]]
        rows = jnp.concatenate(split_two(jnp.concatenate(rows, axis=0)), axis=0)
        both = lax.dot_general(
            rows, planes, (((1,), (1,)), ((), ())), preferred_element_type=F32
        )
        both = both[:80, :] + both[80:, :]
        at = (e >> 4) * (36 * PITCH) + (e & 15)
        for k in range(5):
            even = both[8 * k : 8 * k + 8, :]
            odd = both[40 + 8 * k : 48 + 8 * k, :]
            t = jnp.where(low_half, even, odd)
            t = t + pltpu.roll(jnp.where(low_half, odd, even), 64, 1)
            n = 8 if k < 4 else 4
            parts[pl.ds(at + k * 8 * PITCH, n, stride=PITCH), :] = t[0:n, :]


def own_kernel(elem, group, vel, nodes, field, parts, drag, table, fluid):
    table[...] = nodes[...]
    spread_field(vel, field)
    elements = [elem[r] for r in range(SHARE)]
    interpolate(group, elements, field, nodes, fluid)
    find_drag(group, fluid, drag)
    project(group, elements, drag, nodes, parts)


def element_list(group):
    labels = group[256:257, :].astype(jnp.int32)
    return [labels[0, r] for r in range(SHARE)]


def middle_kernel(group, field, nodes, _, drag, parts, fluid):
    elements = element_list(group)
    interpolate(group, elements, field, nodes, fluid)
    find_drag(group, fluid, drag)
    project(group, elements, drag, nodes, parts)


def rest_kernel(group, field, nodes, _, drag, inside, ghosts, parts, fluid):
    middle_kernel(group, field, nodes, None, drag, parts, fluid)
    gather_parts(parts, inside, ghosts)


def gather_parts(parts, inside, ghosts):
    low_half = lanes() < 64
    odd = lax.axis_index("gx") & 1
    to_lo = (1 - odd) * 12
    to_hi = odd * 12

    def part(x, y, c, k, h):
        n = 2 * c + k if k < 2 else 6 + c
        return parts[pl.ds(((x * 4 + y) * 36 + n * 4 + h) * PITCH, 16), :]

    def one(y, _):
        for c in range(3):
            lower = []
            upper = []
            for h in range(4):
                lo = part(0, y, c, 1, h) + part(1, y, c, 0, h)
                hi = part(1, y, c, 1, h) + part(0, y, c, 2, h)
                inside[c * 8 + y, :, 128 * h : 128 * h + 128] = lo
                inside[c * 8 + 4 + y, :, 128 * h : 128 * h + 128] = hi
                lower.append(lo)
                upper.append(hi)
            for h in range(4):
                lo = part(0, y, c, 0, h)
                hi = part(1, y, c, 2, h)
                if h == 3:
                    lo = lo + jnp.where(low_half, 0.0, pltpu.roll(lower[0], 64, 1))
                if h == 0:
                    hi = hi + jnp.where(low_half, pltpu.roll(upper[3], 64, 1), 0.0)
                ghosts[to_lo + c * 4 + y, :, 128 * h : 128 * h + 128] = lo
                ghosts[to_hi + c * 4 + y, :, 128 * h : 128 * h + 128] = hi
        return 0

    lax.fori_loop(0, 4, one, 0)


def first_pass_kernel(last_gx, inside, sent, near, far, field, faces):
    low_half = lanes() < 64
    spot = (lanes() % 64) // 8
    gx = lax.axis_index("gx")
    odd = (gx & 1) == 1
    has_before = gx > 0
    has_after = gx < last_gx
    to_lo = (1 - (gx & 1)) * 12
    to_hi = (gx & 1) * 12
    y_odd = (lax.axis_index("gy") & 1) == 1

    def cut(ref, at, h):
        return ref[at, :, 128 * h : 128 * h + 128]

    for c in range(3):
        packed = [jnp.zeros((16, 128), F32), jnp.zeros((16, 128), F32)]
        for y in range(4):
            pair = [(cut(near, c * 4 + y, h), cut(far, c * 4 + y, h)) for h in range(4)]
            got_lo = [jnp.where(odd, n, f) for n, f in pair]
            got_hi = [jnp.where(odd, f, n) for n, f in pair]
            lower = [
                cut(inside, c * 8 + y, h) + jnp.where(has_before, got_lo[h], 0.0) for h in range(4)
            ]
            upper = [
                cut(inside, c * 8 + 4 + y, h) + jnp.where(has_after, got_hi[h], 0.0)
                for h in range(4)
            ]
            first = got_lo[0] + pltpu.roll(cut(sent, to_lo + c * 4 + y, 3), 64, 1)
            last = got_hi[3] + pltpu.roll(cut(sent, to_hi + c * 4 + y, 0), 64, 1)
            low3, up0 = lower[3], upper[0]
            lower[0] = jnp.where(low_half & has_before, first, lower[0])
            upper[3] = jnp.where(low_half | jnp.logical_not(has_after), upper[3], last)
            lower[3] = jnp.where(low_half, low3, low3 + pltpu.roll(up0, 64, 1))
            upper[0] = jnp.where(low_half, up0 + pltpu.roll(low3, 64, 1), up0)
            for x, layer in ((0, lower), (1, upper)):
                for h in range(4):
                    field[c * 8 + x * 4 + y, :, 128 * h : 128 * h + 128] = layer[h]
                    k = x * 4 + h
                    if y == 0:
                        moved = pltpu.roll(layer[h], 8 * k, 1) if k else layer[h]
                        packed[0] = jnp.where(spot == k, moved, packed[0])
                    if y == 3:
                        by = (8 * k - 56) % 128
                        moved = pltpu.roll(layer[h], by, 1) if by else layer[h]
                        packed[1] = jnp.where(spot == k, moved, packed[1])
        faces[16 * c : 16 * c + 16, :] = jnp.where(y_odd, packed[0], packed[1])
        faces[48 + 16 * c : 64 + 16 * c, :] = jnp.where(y_odd, packed[1], packed[0])


def last_passes(field, rows, before, after, buf, start):
    lane = lanes()
    bottom = (lane % 64) < 8
    top = (lane % 64) >= 56
    z = lax.broadcasted_iota(jnp.int32, (16, 128), 0)
    lane16 = lanes((16, 128))
    up_here = (lane16 % 8 == 7) & (z < 15)
    down_here = (lane16 % 8 == 0) & (z > 0)

    def one_comp(c, _):
        lo_pack = before(c)
        hi_pack = after(c)
        for x in range(2):
            for y in rows:
                for h in range(4):
                    k = x * 4 + h

                    def at(row):
                        return field[c * 8 + x * 4 + row, :, 128 * h : 128 * h + 128]

                    if y == 3:
                        above = hi_pack if k == 7 else pltpu.roll(hi_pack, 56 - 8 * k, 1)
                    else:
                        above = pltpu.roll(at(y + 1), 56, 1)
                    if y == 0:
                        below = lo_pack if k == 0 else pltpu.roll(lo_pack, 128 - 8 * k, 1)
                    else:
                        below = pltpu.roll(at(y - 1), 72, 1)
                    g = at(y) + jnp.where(top, above, jnp.where(bottom, below, 0.0))
                    above = pltpu.roll(pltpu.roll(g, 7, 1), 15, 0)
                    below = pltpu.roll(pltpu.roll(g, 121, 1), 1, 0)
                    g = g + jnp.where(up_here, above, jnp.where(down_here, below, 0.0))
                    buf[c * 8 + x * 4 + y, :, 128 * h : 128 * h + 128] = g
                start(c * 8 + x * 4 + y)
        return 0

    lax.fori_loop(0, 3, one_comp, 0)


def inner_kernel(block, field, d0, d1, d2, d3, drag, out):
    for k, d in enumerate((d0, d1, d2, d3)):

        def one(r, _):
            drag[pl.ds(block[k * SHARE + r], 3, stride=128), :] = d[pl.ds(r, 3, stride=32), :]
            return 0

        lax.fori_loop(0, SHARE, one, 0, unroll=8)
    last_passes(field, (1, 2), lambda c: None, lambda c: None, out, lambda row: None)


def outer_kernel(field, got1, got3, done, drag_done, drag, out, buf, sem, drag_sem):
    gy = lax.axis_index("gy")
    odd = (gy & 1) == 1
    between = (gy > 0) & (gy < N_GY - 1)
    moves = [
        pltpu.make_async_copy(
            drag_done.at[pl.ds(96 * k, 96)], drag.at[pl.ds(96 * k, 96)], drag_sem.at[k]
        )
        for k in range(4)
    ] + [
        pltpu.make_async_copy(done.at[row], out.at[row], sem.at[row])
        for row in range(24)
        if row % 4 in (1, 2)
    ]
    for move in moves:
        move.start()

    def copy(row):
        return pltpu.make_async_copy(buf.at[row], out.at[row], sem.at[row])

    def face(c, first):
        a = got1[pl.ds(16 * c, 16), :]
        b = jnp.where(between, got3[pl.ds(16 * c, 16), :], 0.0)
        return jnp.where(odd, a, b) if first else jnp.where(odd, b, a)

    last_passes(
        field,
        (0, 3),
        lambda c: face(c, True),
        lambda c: face(c, False),
        buf,
        lambda row: copy(row).start(),
    )
    for move in moves:
        move.wait()
    for row in range(24):
        if row % 4 in (0, 3):
            copy(row).wait()


def swapped(x, axis, partner):
    return lax.ppermute(x, axis, [(i, partner(i)) for i in range(lax.axis_size(axis))])


def swapped_all(x, partner):
    nx, ny = lax.axis_size("gx"), lax.axis_size("gy")
    pairs = []
    for i in range(nx):
        for j in range(ny):
            a, b = partner(i, j)
            pairs.append((i * ny + j, a * ny + b))
    return lax.ppermute(x, ("gx", "gy"), pairs)


def body(velocity, part_pos, part_vel, part_coef, counts, dest, elem):
    pos = part_pos.transpose(1, 0, 2)
    vel = part_vel.transpose(1, 0, 2)
    coef = part_coef.reshape(256, 128)
    nodes = jnp.asarray(node_table())
    send, block, own_elem, velocity_here = call(
        pack_kernel,
        [((N_GY * ROWS, 128), F32, "vmem"), ((128,), jnp.int32, "smem"), ((128,), jnp.int32, "smem"), ((24, 16, 512), BF16, "vmem")],
        [(a, "raw") for a in (dest, counts, elem, pos, vel, coef, velocity.reshape(24, 16, 512))],
        (SMEM((128,), jnp.int32),) * 3
        + (VMEM(pos.shape, F32),) * 2
        + (VMEM(coef.shape, F32), pltpu.SemaphoreType.DMA((10,))),
    )
    own = send[:ROWS]
    groups = {
        k: swapped(send[k * ROWS : (k + 1) * ROWS], "gy", lambda i, k=k: i ^ k) for k in ORDER
    }
    field, parts, drag_own, table = call(
        own_kernel,
        [((8 * 24 * PITCH, 128), F32, "vmem"), ((8 * 36 * PITCH, 128), F32, "vmem"), ((96, 128), F32, "vmem"), (nodes.shape, F32, "vmem")],
        [(own_elem, "smem"), (own, "vmem"), (velocity_here, "vmem"), (nodes, "hbm")],
        (VMEM((96, 128), F32),),
        flops=OWN_FLOPS,
    )
    fluid = (VMEM((96, 128), F32),)
    drags = {}
    for k in ORDER[:2]:
        drags[k], parts = call(
            middle_kernel,
            [((96, 128), F32, "vmem"), ((8 * 36 * PITCH, 128), F32, "vmem")],
            [(a, "vmem") for a in (groups[k], field, table, parts)],
            fluid,
            flops=OWN_FLOPS,
            aliases={3: 1},
        )
    drags[ORDER[2]], inside, ghosts, _ = call(
        rest_kernel,
        [((96, 128), F32, "vmem")]
        + [((24, 16, 512), F32, "vmem")] * 2
        + [((8 * 36 * PITCH, 128), F32, "vmem")],
        [(a, "vmem") for a in (groups[ORDER[2]], field, table, parts)],
        fluid,
        aliases={3: 3},
    )
    last_gx = lax.axis_size("gx") - 1

    def other_chip(i, j):
        k = i + 1 if i & 1 else i - 1
        return (k, j) if 0 <= k <= last_gx else (i, j ^ 1)

    far = swapped_all(ghosts[12:], other_chip)
    near = swapped(ghosts[:12], "gx", lambda i: i ^ 1)
    back = {k: swapped(d, "gy", lambda i, k=k: i ^ k) for k, d in drags.items()}
    last_gx = lax.axis_size("gx") - 1
    field, faces = call(
        lambda *refs: first_pass_kernel(last_gx, *refs),
        [((24, 16, 512), F32, "vmem"), ((96, 128), F32, "vmem")],
        [(inside, "vmem"), (ghosts, "vmem"), (near, "vmem"), (far, "vmem")],
    )
    got1 = swapped(faces[:48], "gy", lambda i: i ^ 1)
    got3 = swapped_all(faces[48:], lambda i, j: (i, j ^ 3) if 0 < j < N_GY - 1 else (i ^ 1, j))
    grid = (24, 16, 512)
    drag, inner = call(
        inner_kernel,
        [((384, 128), F32, "vmem"), (grid, F32, "vmem")],
        [(block, "smem"), (field, "vmem"), (drag_own, "vmem")]
        + [(back[k], "vmem") for k in range(1, N_GY)],
        flops=UNPACK_FLOPS,
    )
    drag, out = call(
        outer_kernel,
        [((384, 128), F32, "raw"), (grid, F32, "raw")],
        [(a, "vmem") for a in (field, got1, got3, inner, drag)],
        (VMEM(grid, F32), pltpu.SemaphoreType.DMA((24,)), pltpu.SemaphoreType.DMA((4,))),
    )
    return (
        drag.reshape(3, 128, 128).transpose(1, 0, 2),
        out.reshape(velocity.shape),
    )


def solution(mesh):
    in_specs = (
        P(None, "gx", "gy", None, None),
        P(("gx", "gy"), None, None),
        P(("gx", "gy"), None, None),
        P(("gx", "gy"), None, None),
        P(("gx", "gy")),
        P(("gx", "gy")),
        P(("gx", "gy")),
    )
    out_specs = (P(("gx", "gy"), None, None), P(None, "gx", "gy", None, None))
    return jax.shard_map(body, mesh=mesh, in_specs=in_specs, out_specs=out_specs, check_vma=False)
```

```python
import jax
import jax.numpy as jnp
import numpy as np
from jax import lax
from jax.experimental import pallas as pl
from jax.experimental.pallas import tpu as pltpu
from jax.sharding import PartitionSpec as P

GLL = (
    -1.0,
    -0.8717401485096066,
    -0.5917001814331423,
    -0.2092992179024789,
    0.2092992179024789,
    0.5917001814331423,
    0.8717401485096066,
    1.0,
)
SHARPNESS = 8.0
INTERPRET = False
F32 = jnp.float32
BF16 = jnp.bfloat16
VMEM = pltpu.VMEM
SMEM = pltpu.SMEM
N_GY = 4
SHARE = 32
ROWS = 264
PAIRED = (0, 2, 4, 6, 1, 3, 5, 7)


def node_table():
    q = np.array(GLL, np.float64)
    rows = []
    for order in (tuple(range(8)), PAIRED):
        for t in range(7):
            rows.append([q[[m for m in range(8) if m != i][t]] for i in order])
        rows.append([1.0 / np.prod([q[i] - q[m] for m in range(8) if m != i]) for i in order])
    rows.append([q[i] for i in range(8)])
    for first, second in ((-2.0, 0.0), (2.0, 2.0)):
        for half in (PAIRED[:4], PAIRED[4:]):
            rows.append([q[i] + first for i in half] + [q[i] + second for i in half])
    table = np.array(rows, np.float32).reshape(-1, 1)
    return np.ascontiguousarray(np.broadcast_to(table, (table.shape[0], 128)))


PITCH = 17
ORDER = (1, 3, 2)
OWN_FLOPS = 2_000_000_000
UNPACK_FLOPS = 1_000_000_000


SPACES = {"vmem": VMEM, "hbm": VMEM, "": VMEM, "smem": SMEM, "table": SMEM, "raw": pltpu.HBM}


def call(kernel, outs, ins, scratch=(), flops=0, aliases=None):
    args = [
        a
        if INTERPRET
        else pltpu.with_memory_space_constraint(a, VMEM if m == "vmem" else pltpu.HBM)
        if m in ("vmem", "hbm", "table", "raw")
        else a
        for a, m in ins
    ]
    shapes = [
        VMEM(shape, dtype) if m == "vmem" and not INTERPRET else jax.ShapeDtypeStruct(shape, dtype)
        for shape, dtype, m in outs
    ]
    return pl.pallas_call(
        kernel,
        out_shape=shapes,
        in_specs=[pl.BlockSpec(memory_space=SPACES[m]) for _, m in ins],
        out_specs=[pl.BlockSpec(memory_space=SPACES[m]) for _, _, m in outs],
        scratch_shapes=scratch,
        interpret=INTERPRET,
        input_output_aliases=aliases or {},
        compiler_params=pltpu.CompilerParams(vmem_limit_bytes=24 * 1024 * 1024),
        cost_estimate=pl.CostEstimate(flops=flops, bytes_accessed=0, transcendentals=0),
    )(*args)


def lanes(shape=(1, 128)):
    return lax.broadcasted_iota(jnp.int32, shape, len(shape) - 1)


def pack_kernel(
    dest_hbm, counts_hbm, elem_hbm, pos_hbm, vel_hbm, coef_hbm, velocity_hbm,
    send, block, own_elem, velocity,
    dest, counts, elem, pos, vel, coef, sem,
):
    tables = [
        pltpu.make_async_copy(a, b, sem.at[k])
        for k, (a, b) in enumerate(((dest_hbm, dest), (counts_hbm, counts), (elem_hbm, elem)))
    ]
    halves = []
    for k in range(2):
        cut = pl.ds(64 * k, 64)
        pairs = (
            (pos_hbm.at[:, cut], pos.at[:, cut]),
            (vel_hbm.at[:, cut], vel.at[:, cut]),
            (coef_hbm.at[pl.ds(128 * k, 128)], coef.at[pl.ds(128 * k, 128)]),
        )
        halves.append(
            [pltpu.make_async_copy(a, b, sem.at[3 + 3 * k + n]) for n, (a, b) in enumerate(pairs)]
        )
    fetch = pltpu.make_async_copy(velocity_hbm, velocity, sem.at[9])
    for copy in tables + halves[0] + halves[1] + [fetch]:
        copy.start()
    me = lax.axis_index("gy")
    lane = lanes()
    ids = lax.broadcasted_iota(jnp.int32, (8, 128), 0) * 128 + lanes((8, 128))

    def one(b, state):
        taken, labels = state
        d = dest[b] ^ me
        r = (taken >> (8 * d)) & 255
        e = elem[b]
        block[d * SHARE + r] = b
        own_elem[d * SHARE + r] = e
        base = d * ROWS + r
        send[pl.ds(base, 3, stride=32), :] = pos[:, b, :]
        send[pl.ds(base + 96, 3, stride=32), :] = vel[:, b, :]
        rate = coef[pl.ds(2 * b, 1), :]
        send[pl.ds(base + 192, 1), :] = jnp.where(lane < counts[b], rate, 0.0)
        send[pl.ds(base + 224, 1), :] = coef[pl.ds(2 * b + 1, 1), :]
        labels = jnp.where(ids == d * 128 + r, e, labels)
        return (taken + (1 << (8 * d)), labels)

    state = (jnp.int32(0), jnp.zeros((8, 128), jnp.int32))
    for copy in tables:
        copy.wait()
    for k in range(2):
        for copy in halves[k]:
            copy.wait()
        state = lax.fori_loop(64 * k, 64 * k + 64, one, state, unroll=8)
    fetch.wait()
    labels = state[1].astype(F32)
    for d in range(N_GY):
        send[d * ROWS + 256 : d * ROWS + 264, :] = jnp.broadcast_to(labels[d : d + 1, :], (8, 128))


def split_two(x):
    high = x.astype(BF16)
    low = (x - high.astype(F32)).astype(BF16)
    return high, low


def lagrange(x, nodes, first):
    out = nodes[8 * (first + 7) : 8 * (first + 8), :]
    for t in range(7):
        out = out * (x - nodes[8 * (first + t) : 8 * (first + t + 1), :])
    return out


def gauss(x, nodes, row):
    d = nodes[8 * row : 8 * row + 8, :] - x
    return jnp.exp(d * d * (-SHARPNESS))


def outer(a, b):
    return jnp.concatenate([a[j : j + 1, :] * b for j in range(8)], axis=0)


def spread_field(vel, field):
    low_half = lanes() < 64

    def one(xy, _):
        for c in range(3):
            for h in range(4):
                t = vel[c * 8 + xy, :, 128 * h : 128 * h + 128].astype(F32)
                turned = pltpu.roll(t, 64, 1)
                at = (xy * 24 + c * 8 + h) * PITCH
                field[pl.ds(at, 16), :] = jnp.where(low_half, t, turned)
                field[pl.ds(at + 4 * PITCH, 16), :] = jnp.where(low_half, turned, t)
        return 0

    lax.fori_loop(0, 8, one, 0)


def interpolate(group, elements, field, nodes, fluid):
    for r in range(SHARE):
        e = elements[r]
        basis_r = lagrange(group[r : r + 1, :], nodes, 8)
        basis_s = lagrange(group[r + 32 : r + 33, :], nodes, 0)
        basis_t = lagrange(group[r + 64 : r + 65, :], nodes, 0)
        high, low = split_two(outer(basis_s, basis_t))
        nodal = field[pl.ds((e >> 4) * (24 * PITCH) + (e & 15), 24, stride=PITCH), :].astype(BF16)
        part = jnp.dot(nodal, jnp.concatenate([high, low], axis=0), preferred_element_type=F32)
        for c in range(3):
            fluid[c * 32 + r : c * 32 + r + 1, :] = jnp.sum(
                part[8 * c : 8 * c + 8, :] * basis_r, axis=0, keepdims=True
            )


def find_drag(group, fluid, drag):
    w = [
        fluid[32 * c : 32 * c + 32, :] - group[96 + 32 * c : 128 + 32 * c, :] for c in range(3)
    ]
    scale = group[224:256, :]
    square = (w[0] * w[0] + w[1] * w[1] + w[2] * w[2]) * (scale * scale)
    power = jnp.where(square > 0.0, jnp.exp(0.3435 * jnp.log(square)), 0.0)
    factor = group[192:224, :] * (1.0 + 0.15 * power)
    for c in range(3):
        drag[32 * c : 32 * c + 32, :] = factor * w[c]


def project(group, elements, drag, nodes, parts):
    low_half = lanes() < 64
    upper_rows = lax.broadcasted_iota(jnp.int32, (8, 128), 0) < 4

    for r in range(SHARE):
        e = elements[r]
        x = group[r : r + 1, :]
        near = [gauss(x, nodes, 17 + k) for k in range(2)]
        after = [gauss(x, nodes, 19 + k) for k in range(2)]
        planes = outer(
            gauss(group[r + 32 : r + 33, :], nodes, 16),
            gauss(group[r + 64 : r + 65, :], nodes, 16),
        )
        planes = jnp.concatenate(split_two(planes), axis=0)
        force = [-drag[c * 32 + r : c * 32 + r + 1, :] for c in range(3)]
        mixed = jnp.where(upper_rows, force[0], force[1])
        rows = []
        for k in range(2):
            rows += [near[k] * f for f in force] + [after[k] * mixed, after[k] * force[2]]
        rows = jnp.concatenate(split_two(jnp.concatenate(rows, axis=0)), axis=0)
        both = lax.dot_general(
            rows, planes, (((1,), (1,)), ((), ())), preferred_element_type=F32
        )
        both = both[:80, :] + both[80:, :]
        at = (e >> 4) * (36 * PITCH) + (e & 15)
        for k in range(5):
            even = both[8 * k : 8 * k + 8, :]
            odd = both[40 + 8 * k : 48 + 8 * k, :]
            t = jnp.where(low_half, even, odd)
            t = t + pltpu.roll(jnp.where(low_half, odd, even), 64, 1)
            n = 8 if k < 4 else 4
            parts[pl.ds(at + k * 8 * PITCH, n, stride=PITCH), :] = t[0:n, :]


def own_kernel(elem, group, vel, nodes, field, parts, drag, table, fluid):
    table[...] = nodes[...]
    spread_field(vel, field)
    elements = [elem[r] for r in range(SHARE)]
    interpolate(group, elements, field, nodes, fluid)
    find_drag(group, fluid, drag)
    project(group, elements, drag, nodes, parts)


def element_list(group):
    labels = group[256:257, :].astype(jnp.int32)
    return [labels[0, r] for r in range(SHARE)]


def middle_kernel(group, field, nodes, _, drag, parts, fluid):
    elements = element_list(group)
    interpolate(group, elements, field, nodes, fluid)
    find_drag(group, fluid, drag)
    project(group, elements, drag, nodes, parts)


def rest_kernel(group, field, nodes, _, drag, inside, ghosts, parts, fluid):
    middle_kernel(group, field, nodes, None, drag, parts, fluid)
    gather_parts(parts, inside, ghosts)


def gather_parts(parts, inside, ghosts):
    low_half = lanes() < 64
    odd = lax.axis_index("gx") & 1
    to_lo = (1 - odd) * 12
    to_hi = odd * 12

    def part(x, y, c, k, h):
        n = 2 * c + k if k < 2 else 6 + c
        return parts[pl.ds(((x * 4 + y) * 36 + n * 4 + h) * PITCH, 16), :]

    def one(y, _):
        for c in range(3):
            lower = []
            upper = []
            for h in range(4):
                lo = part(0, y, c, 1, h) + part(1, y, c, 0, h)
                hi = part(1, y, c, 1, h) + part(0, y, c, 2, h)
                inside[c * 8 + y, :, 128 * h : 128 * h + 128] = lo
                inside[c * 8 + 4 + y, :, 128 * h : 128 * h + 128] = hi
                lower.append(lo)
                upper.append(hi)
            for h in range(4):
                lo = part(0, y, c, 0, h)
                hi = part(1, y, c, 2, h)
                if h == 3:
                    lo = lo + jnp.where(low_half, 0.0, pltpu.roll(lower[0], 64, 1))
                if h == 0:
                    hi = hi + jnp.where(low_half, pltpu.roll(upper[3], 64, 1), 0.0)
                ghosts[to_lo + c * 4 + y, :, 128 * h : 128 * h + 128] = lo
                ghosts[to_hi + c * 4 + y, :, 128 * h : 128 * h + 128] = hi
        return 0

    lax.fori_loop(0, 4, one, 0)


def first_pass_kernel(last_gx, inside, sent, near, far, field, faces):
    low_half = lanes() < 64
    spot = (lanes() % 64) // 8
    gx = lax.axis_index("gx")
    odd = (gx & 1) == 1
    has_before = gx > 0
    has_after = gx < last_gx
    to_lo = (1 - (gx & 1)) * 12
    to_hi = (gx & 1) * 12
    y_odd = (lax.axis_index("gy") & 1) == 1

    def cut(ref, at, h):
        return ref[at, :, 128 * h : 128 * h + 128]

    for c in range(3):
        packed = [jnp.zeros((16, 128), F32), jnp.zeros((16, 128), F32)]
        for y in range(4):
            pair = [(cut(near, c * 4 + y, h), cut(far, c * 4 + y, h)) for h in range(4)]
            got_lo = [jnp.where(odd, n, f) for n, f in pair]
            got_hi = [jnp.where(odd, f, n) for n, f in pair]
            lower = [
                cut(inside, c * 8 + y, h) + jnp.where(has_before, got_lo[h], 0.0) for h in range(4)
            ]
            upper = [
                cut(inside, c * 8 + 4 + y, h) + jnp.where(has_after, got_hi[h], 0.0)
                for h in range(4)
            ]
            first = got_lo[0] + pltpu.roll(cut(sent, to_lo + c * 4 + y, 3), 64, 1)
            last = got_hi[3] + pltpu.roll(cut(sent, to_hi + c * 4 + y, 0), 64, 1)
            low3, up0 = lower[3], upper[0]
            lower[0] = jnp.where(low_half & has_before, first, lower[0])
            upper[3] = jnp.where(low_half | jnp.logical_not(has_after), upper[3], last)
            lower[3] = jnp.where(low_half, low3, low3 + pltpu.roll(up0, 64, 1))
            upper[0] = jnp.where(low_half, up0 + pltpu.roll(low3, 64, 1), up0)
            for x, layer in ((0, lower), (1, upper)):
                for h in range(4):
                    field[c * 8 + x * 4 + y, :, 128 * h : 128 * h + 128] = layer[h]
                    k = x * 4 + h
                    if y == 0:
                        moved = pltpu.roll(layer[h], 8 * k, 1) if k else layer[h]
                        packed[0] = jnp.where(spot == k, moved, packed[0])
                    if y == 3:
                        by = (8 * k - 56) % 128
                        moved = pltpu.roll(layer[h], by, 1) if by else layer[h]
                        packed[1] = jnp.where(spot == k, moved, packed[1])
        faces[16 * c : 16 * c + 16, :] = jnp.where(y_odd, packed[0], packed[1])
        faces[48 + 16 * c : 64 + 16 * c, :] = jnp.where(y_odd, packed[1], packed[0])


def last_passes(field, rows, before, after, buf, start):
    lane = lanes()
    bottom = (lane % 64) < 8
    top = (lane % 64) >= 56
    z = lax.broadcasted_iota(jnp.int32, (16, 128), 0)
    lane16 = lanes((16, 128))
    up_here = (lane16 % 8 == 7) & (z < 15)
    down_here = (lane16 % 8 == 0) & (z > 0)

    def one_comp(c, _):
        lo_pack = before(c)
        hi_pack = after(c)
        for x in range(2):
            for y in rows:
                for h in range(4):
                    k = x * 4 + h

                    def at(row):
                        return field[c * 8 + x * 4 + row, :, 128 * h : 128 * h + 128]

                    if y == 3:
                        above = hi_pack if k == 7 else pltpu.roll(hi_pack, 56 - 8 * k, 1)
                    else:
                        above = pltpu.roll(at(y + 1), 56, 1)
                    if y == 0:
                        below = lo_pack if k == 0 else pltpu.roll(lo_pack, 128 - 8 * k, 1)
                    else:
                        below = pltpu.roll(at(y - 1), 72, 1)
                    g = at(y) + jnp.where(top, above, jnp.where(bottom, below, 0.0))
                    above = pltpu.roll(pltpu.roll(g, 7, 1), 15, 0)
                    below = pltpu.roll(pltpu.roll(g, 121, 1), 1, 0)
                    g = g + jnp.where(up_here, above, jnp.where(down_here, below, 0.0))
                    buf[c * 8 + x * 4 + y, :, 128 * h : 128 * h + 128] = g
                start(c * 8 + x * 4 + y)
        return 0

    lax.fori_loop(0, 3, one_comp, 0)


def inner_kernel(block, field, d0, d1, d2, d3, drag, out):
    for k, d in enumerate((d0, d1, d2, d3)):

        def one(r, _):
            drag[pl.ds(block[k * SHARE + r], 3, stride=128), :] = d[pl.ds(r, 3, stride=32), :]
            return 0

        lax.fori_loop(0, SHARE, one, 0, unroll=8)
    last_passes(field, (1, 2), lambda c: None, lambda c: None, out, lambda row: None)


def outer_kernel(field, got1, got3, done, drag_done, drag, out, buf, sem, drag_sem):
    gy = lax.axis_index("gy")
    odd = (gy & 1) == 1
    between = (gy > 0) & (gy < N_GY - 1)
    moves = [
        pltpu.make_async_copy(
            drag_done.at[pl.ds(96 * k, 96)], drag.at[pl.ds(96 * k, 96)], drag_sem.at[k]
        )
        for k in range(4)
    ] + [
        pltpu.make_async_copy(done.at[row], out.at[row], sem.at[row])
        for row in range(24)
        if row % 4 in (1, 2)
    ]
    for move in moves:
        move.start()

    def copy(row):
        return pltpu.make_async_copy(buf.at[row], out.at[row], sem.at[row])

    def face(c, first):
        a = got1[pl.ds(16 * c, 16), :]
        b = jnp.where(between, got3[pl.ds(16 * c, 16), :], 0.0)
        return jnp.where(odd, a, b) if first else jnp.where(odd, b, a)

    last_passes(
        field,
        (0, 3),
        lambda c: face(c, True),
        lambda c: face(c, False),
        buf,
        lambda row: copy(row).start(),
    )
    for move in moves:
        move.wait()
    for row in range(24):
        if row % 4 in (0, 3):
            copy(row).wait()


def swapped(x, axis, partner):
    return lax.ppermute(x, axis, [(i, partner(i)) for i in range(lax.axis_size(axis))])


def swapped_all(x, partner):
    nx, ny = lax.axis_size("gx"), lax.axis_size("gy")
    pairs = []
    for i in range(nx):
        for j in range(ny):
            a, b = partner(i, j)
            pairs.append((i * ny + j, a * ny + b))
    return lax.ppermute(x, ("gx", "gy"), pairs)


def body(velocity, part_pos, part_vel, part_coef, counts, dest, elem):
    pos = part_pos.transpose(1, 0, 2)
    vel = part_vel.transpose(1, 0, 2)
    coef = part_coef.reshape(256, 128)
    nodes = jnp.asarray(node_table())
    send, block, own_elem, velocity_here = call(
        pack_kernel,
        [((N_GY * ROWS, 128), F32, "vmem"), ((128,), jnp.int32, "smem"), ((128,), jnp.int32, "smem"), ((24, 16, 512), BF16, "vmem")],
        [(a, "raw") for a in (dest, counts, elem, pos, vel, coef, velocity.reshape(24, 16, 512))],
        (SMEM((128,), jnp.int32),) * 3
        + (VMEM(pos.shape, F32),) * 2
        + (VMEM(coef.shape, F32), pltpu.SemaphoreType.DMA((10,))),
    )
    own = send[:ROWS]
    groups = {
        k: swapped(send[k * ROWS : (k + 1) * ROWS], "gy", lambda i, k=k: i ^ k) for k in ORDER
    }
    field, parts, drag_own, table = call(
        own_kernel,
        [((8 * 24 * PITCH, 128), F32, "vmem"), ((8 * 36 * PITCH, 128), F32, "vmem"), ((96, 128), F32, "vmem"), (nodes.shape, F32, "vmem")],
        [(own_elem, "smem"), (own, "vmem"), (velocity_here, "vmem"), (nodes, "hbm")],
        (VMEM((96, 128), F32),),
        flops=OWN_FLOPS,
    )
    fluid = (VMEM((96, 128), F32),)
    drags = {}
    for k in ORDER[:2]:
        drags[k], parts = call(
            middle_kernel,
            [((96, 128), F32, "vmem"), ((8 * 36 * PITCH, 128), F32, "vmem")],
            [(a, "vmem") for a in (groups[k], field, table, parts)],
            fluid,
            flops=OWN_FLOPS,
            aliases={3: 1},
        )
    drags[ORDER[2]], inside, ghosts, _ = call(
        rest_kernel,
        [((96, 128), F32, "vmem")]
        + [((24, 16, 512), F32, "vmem")] * 2
        + [((8 * 36 * PITCH, 128), F32, "vmem")],
        [(a, "vmem") for a in (groups[ORDER[2]], field, table, parts)],
        fluid,
        aliases={3: 3},
    )
    last_gx = lax.axis_size("gx") - 1

    def other_chip(i, j):
        k = i + 1 if i & 1 else i - 1
        return (k, j) if 0 <= k <= last_gx else (i, j ^ 1)

    far = swapped_all(ghosts[12:], other_chip)
    near = swapped(ghosts[:12], "gx", lambda i: i ^ 1)
    back = {k: swapped(d, "gy", lambda i, k=k: i ^ k) for k, d in drags.items()}
    last_gx = lax.axis_size("gx") - 1
    field, faces = call(
        lambda *refs: first_pass_kernel(last_gx, *refs),
        [((24, 16, 512), F32, "vmem"), ((96, 128), F32, "vmem")],
        [(inside, "vmem"), (ghosts, "vmem"), (near, "vmem"), (far, "vmem")],
    )
    got1 = swapped(faces[:48], "gy", lambda i: i ^ 1)
    got3 = swapped_all(faces[48:], lambda i, j: (i, j ^ 3) if 0 < j < N_GY - 1 else (i ^ 1, j))
    grid = (24, 16, 512)
    drag, inner = call(
        inner_kernel,
        [((384, 128), F32, "vmem"), (grid, F32, "vmem")],
        [(block, "smem"), (field, "vmem"), (drag_own, "vmem")]
        + [(back[k], "vmem") for k in range(1, N_GY)],
        flops=UNPACK_FLOPS,
    )
    drag, out = call(
        outer_kernel,
        [((384, 128), F32, "raw"), (grid, F32, "raw")],
        [(a, "vmem") for a in (field, got1, got3, inner, drag)],
        (VMEM(grid, F32), pltpu.SemaphoreType.DMA((24,)), pltpu.SemaphoreType.DMA((4,))),
    )
    return (
        drag.reshape(3, 128, 128).transpose(1, 0, 2),
        out.reshape(velocity.shape),
    )


def solution(mesh):
    in_specs = (
        P(None, "gx", "gy", None, None),
        P(("gx", "gy"), None, None),
        P(("gx", "gy"), None, None),
        P(("gx", "gy"), None, None),
        P(("gx", "gy")),
        P(("gx", "gy")),
        P(("gx", "gy")),
    )
    out_specs = (P(("gx", "gy"), None, None), P(None, "gx", "gy", None, None))
    return jax.shard_map(body, mesh=mesh, in_specs=in_specs, out_specs=out_specs, check_vma=False)
```
